128 devices in a mesh: tm: 16 (over z, y), col: 8 (over x, core).
Axes of the slice: x: 4, y: 4, z: 4, core: 2. Of those that a mesh axis runs over, the one named last changes fastest.
Arguments:
- block_values: bfloat16 [8, 32768, 128], P('col', 'tm'), may hold values from -6 to 6
- block_shifts: bfloat16 [8, 32768, 128], P('col', 'tm'), may hold values from -1 to 1
- block_sensor: int32 [8, 32768], P('col', 'tm'), may hold values from 0 to 2047
- block_window: int32 [8, 32768], P('col', 'tm'), may hold values from 0 to 3
- block_owner: int32 [8, 32768, 1], P('col', 'tm'), may hold values from 0 to 15; in each aligned block of 2048 rows (0 to 2047, 2048 to 4095, ..., all dimensions but the last counted through in order) at most 192 rows name the same one
- block_counts: int32 [8, 16], P('col', 'tm'), may hold values from 1536 to 2048
- calibration: bfloat16 [16384, 4096], P('tm', 'col'), may hold values from -0.046875 to 0.046875
Outputs:
- calibrated: bfloat16 [8192, 4096], P('tm', 'col')
The draws below stay inside these ranges and needn't reach their ends.
Inputs may be any that keep to these rules, and one draw needn't show every extreme that they name: `block_owner`: among the 2048 block slots of one device, at most 192 name the same owner, a bound that some block reaches. The live blocks of device (tm t, col c) are its first block_counts[c, t] slots.
All inputs are finite; a program needn't handle non-finite values.
Results may differ from the reference program's by a relative error of at most 0.015.
Values may be sent and summed in bfloat16 or wider, within the bound.
A program may use at most 128 MiB of HBM per device.

```python
import math
import jax
import jax.numpy as jnp
import numpy as np
from jax import lax

SENSORS = 16384
OUTPUTS = 4096
BLOCK_LEN = 128
BLOCKS_DEV = 2048
WINDOWS = 4
CAPACITY = 192
GROUP_SENSORS = 2048
BLOCK_ROWS = 32768
GRID_ROWS = 8192
N_TM = 16
N_COL = 8


def plant(drawn, key, low, high):
    extent = drawn.shape
    index_at = [jax.random.randint(jax.random.fold_in(key, axis), (), 0, extent[axis]) for axis in range(len(extent))]
    drawn = drawn.at[tuple(index_at)].set(low)
    longest = extent.index(max(extent))
    index_at[longest] = (index_at[longest] + 1) % extent[longest]
    return drawn.at[tuple(index_at)].set(high)


def steps_of(key, dims, shards, low, top_value):
    level, own = 1.0, jax.random.fold_in(key, 6)
    for dim, blocks in shards:
        draws = jnp.exp(jax.random.uniform(jax.random.fold_in(own, dim), (blocks,), jnp.float32, low / len(shards), top_value / len(shards)))
        level = level * jnp.repeat(draws, dims[dim] // blocks).reshape([-1 if axis == dim else 1 for axis in range(len(dims))])
    return level


def deal_out(stream_key, own, number, rows, count, top, reach, slope):
    sequence = jax.random.permutation(stream_key, count)
    packed, usual = load_shares(count, rows * top, reach, slope, True), load_shares(count, rows * top, reach, slope, False)
    places = jnp.arange(count)

    def named(lengths, offset_by):
        used = int((lengths > 0).sum())
        fixed = max(1, used // 4)
        shifted = fixed + (places - fixed + offset_by * (used - fixed)) % max(1, count - fixed)
        return jnp.zeros((count,), jnp.int32).at[sequence[jnp.where(places < fixed, places, shifted)]].set(jnp.asarray(lengths, jnp.int32))

    lengths = jnp.where(number % 4 == 0, named(packed, number // 4), named(usual, number - number // 4 - 1))
    mixed = jax.random.permutation(jax.random.fold_in(own, 3), count)
    donor, sink = mixed[0:count // 2 * 2:2], mixed[1:count // 2 * 2:2]
    margin = jnp.minimum(lengths[donor] - 1, reach - lengths[sink]) // 2
    margin = jnp.where((donor == sequence[0]) | (sink == sequence[0]) | (lengths[sink] == 0), 0, jnp.maximum(margin, 0))
    shifted = jax.random.randint(jax.random.fold_in(own, 4), (count // 2,), 0, 1 << 20) % (margin + 1)
    lengths = lengths.at[donor].add(-shifted).at[sink].add(shifted)
    members = jnp.searchsorted(jnp.cumsum(lengths), jnp.arange(rows * top), side="right").astype(jnp.int32)
    grid = members.reshape(top, rows).T
    grid = grid[jax.random.permutation(jax.random.fold_in(own, 1), rows)]
    offset_by = jax.random.randint(jax.random.fold_in(own, 2), (rows, 1), 0, top)
    return jnp.take_along_axis(grid, (jnp.arange(top)[None, :] + offset_by) % top, axis=1)


def load_shares(count, total, bound, skew, full):
    portions = [(1 << 20) // math.isqrt(grade ** skew) + 1 for grade in range(1, count + 1)]
    largest = bound if full else min(bound, max(-(-total // count), total * portions[0] // sum(portions)))
    least = 1 if total - largest >= count - 1 else 0
    holding, spare = [largest] + [least] * (count - 1), total - largest - least * (count - 1)
    while spare > 0:
        free = [i for i in range(1, count) if holding[i] < largest] or [i for i in range(1, count) if holding[i] < bound]
        mass, remaining = sum([portions[i] for i in free]), spare
        for i in free:
            addition = min(bound - holding[i], max(1, remaining * portions[i] // mass), spare)
            holding[i] = holding[i] + addition
            spare = spare - addition
    return np.array(holding)


def gaussian(stream_key, extent, scale, bound, split=(), dtype=jnp.bfloat16):
    level = steps_of(stream_key, extent, split, -0.22, 0.18) if split else 1.0
    values = jax.random.normal(stream_key, extent, jnp.float32) * scale * level
    return jnp.minimum(jnp.maximum(values, -bound), bound).astype(dtype)


def setup_inputs(seed: int = 0) -> dict:
    key_of = jax.random.split(jax.random.key(seed), 8)
    block_values = gaussian(key_of[0], (N_COL, BLOCK_ROWS, BLOCK_LEN), 1.0, 6.0, ((0, 8), (1, 16)))
    block_shifts = jnp.clip(jax.random.uniform(key_of[1], (N_COL, BLOCK_ROWS, BLOCK_LEN), jnp.float32, -1.0, 1.0) * steps_of(key_of[1], (N_COL, BLOCK_ROWS, BLOCK_LEN), ((0, 8), (1, 16)), -0.4, 0.0), -1.0, 1.0).astype(jnp.bfloat16)
    block_sensor = plant(jax.random.randint(key_of[2], (N_COL, BLOCK_ROWS), 0, GROUP_SENSORS), jax.random.fold_in(key_of[2], 1), 0, GROUP_SENSORS - 1).astype(jnp.int32)
    block_window = plant(jax.random.randint(key_of[3], (N_COL, BLOCK_ROWS), 0, WINDOWS), jax.random.fold_in(key_of[3], 1), 0, WINDOWS - 1).astype(jnp.int32)
    block_owner_keys = jax.random.split(jax.random.fold_in(key_of[4], 1), N_COL * BLOCK_ROWS // BLOCKS_DEV)
    block_owner_turns = jax.random.permutation(jax.random.fold_in(key_of[4], 3), N_COL * BLOCK_ROWS // BLOCKS_DEV)
    block_owner = jax.vmap(lambda own, number: deal_out(jax.random.fold_in(key_of[4], 2), own, number, BLOCKS_DEV, N_TM, 1, CAPACITY, 2))(block_owner_keys, block_owner_turns).reshape((N_COL, BLOCK_ROWS, 1))
    block_counts = plant(jax.random.randint(key_of[5], (N_COL, N_TM), 3 * BLOCKS_DEV // 4, BLOCKS_DEV + 1), jax.random.fold_in(key_of[5], 1), 3 * BLOCKS_DEV // 4, BLOCKS_DEV).astype(jnp.int32)
    calibration = gaussian(key_of[6], (SENSORS, OUTPUTS), SENSORS ** -0.5, 0.046875, ((0, 16), (1, 8)))
    return dict(block_values=block_values, block_shifts=block_shifts, block_sensor=block_sensor, block_window=block_window, block_owner=block_owner, block_counts=block_counts, calibration=calibration)


def spread_samples(values, shifts):
    samples = values.astype(jnp.float32)
    offsets = shifts.astype(jnp.float32)
    result = jnp.zeros(samples.shape, jnp.float32)
    lead = [(0, 0)] * (samples.ndim - 1)
    for displace in (-1, 0, 1):
        weight = jnp.maximum(0.0, 1.0 - jnp.abs(offsets - displace)).astype(jnp.bfloat16)
        weight = lax.optimization_barrier(weight).astype(jnp.float32)
        product = weight * samples
        if displace == 1:
            result = result + jnp.pad(product[..., :-1], lead + [(1, 0)])
        elif displace == -1:
            result = result + jnp.pad(product[..., 1:], lead + [(0, 1)])
        else:
            result = result + product
    return result


def reference(block_values, block_shifts, block_sensor, block_window, block_owner, block_counts, calibration):
    length = block_values.shape[2]
    local_index = lax.broadcasted_iota(jnp.int32, (N_COL, BLOCK_ROWS), 1) % BLOCKS_DEV
    counts_rep = jnp.repeat(block_counts, BLOCKS_DEV, axis=1)
    is_live = (local_index < counts_rep).astype(jnp.float32)
    contribution = spread_samples(block_values, block_shifts) * is_live[:, :, None]
    col_base = lax.broadcasted_iota(jnp.int32, (N_COL, BLOCK_ROWS), 0) * GROUP_SENSORS
    row_keys = (block_owner[:, :, 0] * WINDOWS + block_window) * SENSORS + col_base + block_sensor
    summed = jnp.zeros((N_TM * WINDOWS * SENSORS, length), jnp.float32)
    summed = summed.at[row_keys.reshape(-1)].add(contribution.reshape(-1, length))
    aligned = summed.reshape(N_TM * WINDOWS, SENSORS, length).transpose(0, 2, 1)
    aligned = aligned.reshape(GRID_ROWS, SENSORS).astype(jnp.bfloat16)
    return jnp.dot(aligned, calibration, preferred_element_type=jnp.float32).astype(jnp.bfloat16)
```

```python
import jax
import jax.numpy as jnp
from jax import lax
from jax.experimental import pallas as pl
from jax.experimental.pallas import tpu as pltpu
from jax.sharding import Mesh
from jax.sharding import PartitionSpec as P

MESH = pl.DeviceIdType.MESH
F32 = jnp.float32
BF16 = jnp.bfloat16

LENGTH = 128
BLOCKS = 2048
OWNERS = 16
CAPACITY = 192
WINDOWS = 4
GROUP = 2048
ROWS = 512
COLS = 512
CAL_ROWS = 1024
HALF = CAL_ROWS // 2
MSG_ROWS = CAPACITY + 16
SLOTS = OWNERS * CAPACITY
CHUNK = 256
NT = (((1,), (1,)), ((), ()))


def kernel(
    values_ref,
    shifts_ref,
    sensor_ref,
    window_ref,
    owner_ref,
    cal_ref,
    out_ref,
    ranks,
    contrib,
    keys,
    outbuf,
    rx,
    placed,
    slot_sensor,
    aligned,
    calbuf,
    acc,
    give,
    take,
    a2a_s,
    a2a_r,
    x_s,
    x_r,
    cal_s,
    cal_r,
    d2d_s,
    d2d_r,
    ex_s,
    ex_r,
    own_sem,
):
    z, y, x, c = (lax.axis_index(name) for name in ("z", "y", "x", "c"))
    zp, zm, zo = (z + 1) % 4, (z + 3) % 4, (z + 2) % 4
    xp, xm, xo = (x + 1) % 4, (x + 3) % 4, (x + 2) % 4
    y2 = y % 2
    yq = y + 1 - 2 * y2
    sib = 1 - c
    me_t = z * 4 + y

    def piece(zz, row, half):
        return calbuf.at[c, zz * 2 + row, pl.ds(half * HALF, HALF), :]

    def own_piece(half):
        return cal_ref.at[pl.ds(half * HALF, HALF), :]

    def cal_copy(src, dst, sem, device):
        return pltpu.make_async_remote_copy(
            src_ref=src,
            dst_ref=dst,
            send_sem=cal_s.at[sem],
            recv_sem=cal_r.at[sem],
            device_id=device,
            device_id_type=MESH,
        )

    up, down, across = (zp, y, x, c), (zm, y, x, c), (z, yq, x, c)

    def send_up(k):
        src = (
            own_piece(0),
            own_piece(1),
            piece(zm, y2, 0),
            piece(z, 1 - y2, 0),
            piece(zm, 1 - y2, 0),
        )[k]
        dst = (
            piece(z, y2, 0),
            piece(z, y2, 1),
            piece(zm, y2, 0),
            piece(z, 1 - y2, 0),
            piece(zm, 1 - y2, 0),
        )[k]
        return cal_copy(src, dst, k, up)

    def send_down(k):
        src = (
            own_piece(1),
            own_piece(0),
            piece(zp, y2, 1),
            piece(z, 1 - y2, 1),
            piece(zp, 1 - y2, 1),
        )[k]
        dst = (
            piece(z, y2, 1),
            piece(z, y2, 0),
            piece(zp, y2, 1),
            piece(z, 1 - y2, 1),
            piece(zp, 1 - y2, 1),
        )[k]
        return cal_copy(src, dst, 5 + k, down)

    def send_across(k):
        src = (own_piece(0), own_piece(1), piece(zm, y2, 1), piece(zp, y2, 0))[k]
        dst = (piece(z, y2, 0), piece(z, y2, 1), piece(zm, y2, 1), piece(zp, y2, 0))[k]
        return cal_copy(src, dst, 10 + k, across)

    from_below = (
        (zm, y2, 0),
        (zm, y2, 1),
        (zo, y2, 0),
        (zm, 1 - y2, 0),
        (zo, 1 - y2, 0),
    )
    from_above = (
        (zp, y2, 1),
        (zp, y2, 0),
        (zo, y2, 1),
        (zp, 1 - y2, 1),
        (zo, 1 - y2, 1),
    )
    from_across = ((z, 1 - y2, 0), (z, 1 - y2, 1), (zm, 1 - y2, 1), (zp, 1 - y2, 0))

    def share(src, zz, row, half):
        at = (zz * 2 + row) * 2 + half
        return pltpu.make_async_remote_copy(
            src_ref=src,
            dst_ref=piece(zz, row, half),
            send_sem=d2d_s.at[at],
            recv_sem=d2d_r.at[at],
            device_id=(z, y, x, sib),
            device_id_type=MESH,
        )

    def arrive(sem, where, device):
        spot = piece(*where)
        cal_copy(spot, spot, sem, device).wait_recv()
        share(spot, *where).start()

    def arrive_below(k):
        arrive(k, from_below[k], down)

    def arrive_above(k):
        arrive(5 + k, from_above[k], up)

    def arrive_across(k):
        arrive(10 + k, from_across[k], across)

    own_copy = pltpu.make_async_copy(cal_ref, calbuf.at[c, z * 2 + y2], own_sem)

    send_up(0).start()
    send_down(0).start()
    send_across(0).start()
    own_copy.start()

    owner_row = owner_ref[...]
    mask = owner_row == lax.broadcasted_iota(jnp.int32, (OWNERS, BLOCKS), 0)
    maskf = mask.astype(F32)
    steps = BLOCKS // 128
    stack = jnp.concatenate(
        [maskf[:, j * 128 : (j + 1) * 128] for j in range(steps)], axis=0
    ).astype(BF16)
    row_id = lax.broadcasted_iota(jnp.int32, (128, 128), 0)
    col_id = lax.broadcasted_iota(jnp.int32, (128, 128), 1)
    strict = (row_id < col_id).astype(F32).astype(BF16)
    before = jnp.dot(stack, strict, preferred_element_type=F32)
    total = jnp.dot(stack, jnp.ones((128, 128), BF16), preferred_element_type=F32)
    offset = jnp.zeros((OWNERS, 128), F32)
    for j in range(steps):
        rank = before[j * OWNERS : (j + 1) * OWNERS] + offset
        ranks[:, j * 128 : (j + 1) * 128] = jnp.where(
            mask[:, j * 128 : (j + 1) * 128], rank.astype(jnp.int32), -1
        )
        offset = offset + total[j * OWNERS : (j + 1) * OWNERS]

    sensor = sensor_ref[...]
    kid = lax.broadcasted_iota(jnp.int32, (16, BLOCKS), 0)
    key_rows = jnp.where(
        kid == 0,
        sensor // 128,
        jnp.where(kid == 1, sensor % 128, jnp.where(kid == 2, window_ref[...], 0)),
    )
    keys[...] = key_rows.astype(F32).astype(BF16)

    lane = lax.broadcasted_iota(jnp.int32, (CHUNK, LENGTH), 1)

    @pl.loop(0, BLOCKS // CHUNK)
    def _(i):
        at = pl.ds(pl.multiple_of(i * CHUNK, CHUNK), CHUNK)
        samples = values_ref[at, :].astype(F32)
        offsets = shifts_ref[at, :].astype(F32)

        def product(k):
            weight = jnp.maximum(0.0, 1.0 - jnp.abs(offsets - k)).astype(BF16)
            return weight.astype(F32) * samples

        result = product(0.0)
        result = result + jnp.where(lane >= 1, pltpu.roll(product(1.0), 1, 1), 0.0)
        result = result + jnp.where(
            lane < LENGTH - 1, pltpu.roll(product(-1.0), LENGTH - 1, 1), 0.0
        )
        contrib[at, :] = result.astype(BF16)

    def destination(k):
        zd = (z + k // 4) % 4
        cd = k % 2
        yd = 2 * c + (k // 2) % 2
        yo = yd + cd * (3 - 2 * yd)
        return zd, yd, cd, zd * 4 + yo

    def message_copy(k, zd, yd, cd):
        return pltpu.make_async_remote_copy(
            src_ref=outbuf.at[k],
            dst_ref=rx.at[x, me_t],
            send_sem=a2a_s.at[k],
            recv_sem=a2a_r.at[me_t],
            device_id=(zd, yd, x, cd),
            device_id_type=MESH,
        )

    slot = lax.broadcasted_iota(jnp.int32, (256, BLOCKS), 0)
    slot = jnp.where(slot >= CAPACITY, slot - 64, slot)

    @pl.loop(0, OWNERS)
    def _(k):
        zd, yd, cd, owner = destination(k)
        pick = (ranks[pl.ds(owner, 1), :] == slot).astype(F32).astype(BF16)
        rows = jnp.dot(pick[:CAPACITY], contrib[...], preferred_element_type=F32)
        outbuf[k, 0:CAPACITY, :] = rows.astype(BF16)
        tags = lax.dot_general(keys[...], pick, NT, preferred_element_type=F32)
        tags = jnp.concatenate([tags[0:8, 0:128], tags[0:8, 128:256]], axis=0)
        outbuf[k, CAPACITY:MSG_ROWS, :] = tags.astype(BF16)
        is_self = (zd == z) & (yd == y) & (cd == c)

        @pl.when(jnp.logical_not(is_self))
        def _():
            message_copy(k, zd, yd, cd).start()

        @pl.when(is_self)
        def _():
            pltpu.make_async_copy(
                outbuf.at[k], rx.at[x, me_t], a2a_r.at[me_t]
            ).start()

    send_up(1).start()
    send_down(1).start()
    send_across(1).start()
    share(own_piece(0), z, y2, 0).start()
    share(own_piece(1), z, y2, 1).start()

    arrive_below(0)
    send_up(2).start()
    arrive_across(0)
    send_up(3).start()
    arrive_above(0)
    send_down(2).start()

    def x_copy(src_x, half, sem, device):
        span = rx.at[src_x, pl.ds(half * 8, 8)]
        return pltpu.make_async_remote_copy(
            src_ref=span,
            dst_ref=span,
            send_sem=x_s.at[sem],
            recv_sem=x_r.at[sem],
            device_id=device,
            device_id_type=MESH,
        )

    right, left = (z, y, xp, c), (z, y, xm, c)

    def message_wait(t):
        pltpu.make_async_copy(rx.at[x, t], rx.at[x, t], a2a_r.at[t]).wait()

    @pl.loop(0, 8)
    def _(t):
        message_wait(t)

    x_copy(x, 0, 0, right).start()

    @pl.loop(8, 16)
    def _(t):
        message_wait(t)

    x_copy(x, 1, 3, left).start()
    x_copy(x, 1, 1, right).start()
    x_copy(x, 0, 2, left).start()

    low_lanes = lax.broadcasted_iota(jnp.int32, (1, 128), 1) < 64

    def place(q):
        @pl.loop(0, OWNERS // 2)
        def _(p):
            m0 = rx.at[q, 2 * p]
            m1 = rx.at[q, 2 * p + 1]
            k0 = m0[CAPACITY:MSG_ROWS, :].astype(F32)
            k1 = m1[CAPACITY:MSG_ROWS, :].astype(F32)
            joint = jnp.where(low_lanes, k0[8:16], k1[8:16])
            tiles = (
                (m0[0:128, :], k0[0:8]),
                (m1[0:128, :], k1[0:8]),
                (
                    jnp.concatenate([m0[128:CAPACITY, :], m1[128:CAPACITY, :]], axis=0),
                    joint,
                ),
            )
            for n, (rows, tags) in enumerate(tiles):
                at = pl.ds(pl.multiple_of(p * 384 + n * 128, 128), 128)
                turned = rows.astype(F32).T
                slot_sensor[0:1, at] = (tags[0:1] * 128.0 + tags[1:2]).astype(jnp.int32)
                for w in range(WINDOWS):
                    placed[w * 128 : (w + 1) * 128, at] = jnp.where(
                        tags[2:3] == float(w), turned, 0.0
                    ).astype(BF16)

        @pl.loop(0, GROUP // CHUNK)
        def _(j):
            ids = lax.broadcasted_iota(jnp.int32, (CHUNK, SLOTS), 0) + j * CHUNK
            hot = (ids == slot_sensor[0:1, :]).astype(F32).astype(BF16)
            block = lax.dot_general(placed[...], hot, NT, preferred_element_type=F32)
            at = pl.ds(pl.multiple_of(j * CHUNK, CHUNK), CHUNK)
            aligned[q, :, at] = block.astype(BF16)

    place(x)

    arrive_below(1)
    arrive_above(1)
    send_across(2).start()
    send_across(3).start()
    arrive_across(1)
    send_down(3).start()

    x_copy(xm, 0, 0, left).wait_recv()
    x_copy(xm, 0, 4, right).start()
    x_copy(xp, 1, 3, right).wait_recv()
    x_copy(xp, 1, 5, left).start()
    x_copy(xm, 1, 1, left).wait_recv()
    place(xm)

    arrive_below(2)
    arrive_above(2)
    arrive_across(2)

    x_copy(xp, 0, 2, right).wait_recv()
    place(xp)

    arrive_below(3)
    send_up(4).start()
    arrive_above(3)
    send_down(4).start()
    arrive_across(3)

    x_copy(xo, 0, 4, left).wait_recv()
    x_copy(xo, 1, 5, right).wait_recv()
    place(xo)

    own_copy.wait()

    def shared(zz, row):
        for half in range(2):
            at = (zz * 2 + row) * 2 + half
            spot = calbuf.at[sib, zz * 2 + row, pl.ds(half * HALF, HALF), :]
            pltpu.make_async_remote_copy(
                src_ref=spot,
                dst_ref=spot,
                send_sem=d2d_s.at[at],
                recv_sem=d2d_r.at[at],
                device_id=(z, y, x, sib),
                device_id_type=MESH,
            ).wait_recv()

    acc[...] = jnp.zeros_like(acc)

    def multiply(zz):
        @pl.loop(0, 4)
        def _(it):
            row, panel = it // 2, it % 2
            at = pl.ds(pl.multiple_of(row * CAL_ROWS, CAL_ROWS), CAL_ROWS)
            acc[panel] += jnp.dot(
                aligned[zz, :, at], calbuf[panel, zz * 2 + row], preferred_element_type=F32
            )

    for zz in (z, zm, zp):
        shared(zz, 0)
        shared(zz, 1)
        multiply(zz)

    arrive_below(4)
    arrive_above(4)
    shared(zo, 0)
    shared(zo, 1)
    multiply(zo)

    give[...] = acc[...].astype(BF16)

    def exchange(panel, sem_s, sem_r, device):
        return pltpu.make_async_remote_copy(
            src_ref=give.at[panel],
            dst_ref=take.at[sem_r],
            send_sem=ex_s.at[sem_s],
            recv_sem=ex_r.at[sem_r],
            device_id=device,
            device_id_type=MESH,
        )

    @pl.when(c == 0)
    def _():
        over = exchange(1, 0, 0, (z, y, x, 1))
        over.start()
        exchange(0, 0, 0, (z, 3 - y, x, 1)).wait_recv()
        out_ref[...] = (acc[0] + take[0].astype(F32)).astype(BF16)
        over.wait_send()

    @pl.when(c == 1)
    def _():
        first = exchange(0, 0, 0, (z, 3 - y, x, 0))
        first.start()
        second = exchange(1, 1, 1, (z, 3 - y, x, 1))
        second.start()
        exchange(0, 0, 0, (z, y, x, 0)).wait_recv()
        exchange(1, 1, 1, (z, 3 - y, x, 1)).wait_recv()
        out_ref[...] = (take[0].astype(F32) + take[1].astype(F32)).astype(BF16)
        first.wait_send()
        second.wait_send()

    for k in range(5):
        send_up(k).wait_send()
        send_down(k).wait_send()
    for k in range(4):
        send_across(k).wait_send()
    share(own_piece(0), z, y2, 0).wait_send()
    share(own_piece(1), z, y2, 1).wait_send()
    for where in from_below + from_above + from_across:
        share(piece(*where), *where).wait_send()
    x_copy(x, 0, 0, right).wait_send()
    x_copy(x, 1, 1, right).wait_send()
    x_copy(x, 0, 2, left).wait_send()
    x_copy(x, 1, 3, left).wait_send()
    x_copy(xm, 0, 4, right).wait_send()
    x_copy(xp, 1, 5, left).wait_send()

    @pl.loop(0, OWNERS)
    def _(k):
        zd, yd, cd, _owner = destination(k)

        @pl.when(jnp.logical_not((zd == z) & (yd == y) & (cd == c)))
        def _():
            message_copy(k, zd, yd, cd).wait_send()


def per_device(
    block_values, block_shifts, block_sensor, block_window, block_owner, block_counts, calibration
):
    index = lax.broadcasted_iota(jnp.int32, (1, BLOCKS), 1)
    owner = jnp.where(index < block_counts[0, 0], block_owner.reshape(1, BLOCKS), -1)
    vmem = pl.BlockSpec(memory_space=pltpu.VMEM)
    return pl.pallas_call(
        kernel,
        out_shape=jax.ShapeDtypeStruct((ROWS, COLS), BF16),
        in_specs=[vmem] * 5 + [pl.BlockSpec(memory_space=pl.ANY)],
        out_specs=vmem,
        scratch_shapes=[
            pltpu.VMEM((OWNERS, BLOCKS), jnp.int32),
            pltpu.VMEM((BLOCKS, LENGTH), BF16),
            pltpu.VMEM((16, BLOCKS), BF16),
            pltpu.VMEM((OWNERS, MSG_ROWS, LENGTH), BF16),
            pltpu.VMEM((4, OWNERS, MSG_ROWS, LENGTH), BF16),
            pltpu.VMEM((ROWS, SLOTS), BF16),
            pltpu.VMEM((8, SLOTS), jnp.int32),
            pltpu.VMEM((4, ROWS, GROUP), BF16),
            pltpu.VMEM((2, 8, CAL_ROWS, COLS), BF16),
            pltpu.VMEM((2, ROWS, COLS), F32),
            pltpu.VMEM((2, ROWS, COLS), BF16),
            pltpu.VMEM((2, ROWS, COLS), BF16),
            pltpu.SemaphoreType.DMA((OWNERS,)),
            pltpu.SemaphoreType.DMA((OWNERS,)),
            pltpu.SemaphoreType.DMA((6,)),
            pltpu.SemaphoreType.DMA((6,)),
            pltpu.SemaphoreType.DMA((14,)),
            pltpu.SemaphoreType.DMA((14,)),
            pltpu.SemaphoreType.DMA((16,)),
            pltpu.SemaphoreType.DMA((16,)),
            pltpu.SemaphoreType.DMA((2,)),
            pltpu.SemaphoreType.DMA((2,)),
            pltpu.SemaphoreType.DMA,
        ],
        compiler_params=pltpu.CompilerParams(
            has_side_effects=True, vmem_limit_bytes=60 * 1024 * 1024
        ),
    )(
        block_values[0],
        block_shifts[0],
        block_sensor,
        block_window,
        owner,
        calibration,
    )


def solution(mesh):
    torus = Mesh(mesh.devices.reshape(4, 4, 4, 2), ("z", "y", "x", "c"))
    tm, col = ("z", "y"), ("x", "c")
    in_specs = (
        P(col, tm, None),
        P(col, tm, None),
        P(col, tm),
        P(col, tm),
        P(col, tm, None),
        P(col, tm),
        P(tm, col),
    )
    return jax.shard_map(
        per_device, mesh=torus, in_specs=in_specs, out_specs=P(tm, col), check_vma=False
    )
```

```python
import jax
import jax.numpy as jnp
from jax import lax
from jax.experimental import pallas as pl
from jax.experimental.pallas import tpu as pltpu
from jax.sharding import Mesh
from jax.sharding import PartitionSpec as P

MESH = pl.DeviceIdType.MESH
F32 = jnp.float32
BF16 = jnp.bfloat16

LENGTH = 128
BLOCKS = 2048
OWNERS = 16
CAPACITY = 192
WINDOWS = 4
GROUP = 2048
ROWS = 512
COLS = 512
CAL_ROWS = 1024
HALF = CAL_ROWS // 2
PAYLOAD = LENGTH + 16
MSG_ROWS = PAYLOAD + PAYLOAD // 2
SLOTS = OWNERS * CAPACITY
CHUNK = 256
WIDE = 1024
NT = (((1,), (1,)), ((), ()))


def kernel(
    values_ref,
    shifts_ref,
    sensor_ref,
    window_ref,
    owner_ref,
    count_ref,
    cal_ref,
    out_ref,
    ranks,
    payload,
    outbuf,
    rx,
    placed,
    slot_sensor,
    hot,
    aligned,
    calbuf,
    acc,
    give,
    take,
    a2a_s,
    a2a_r,
    x_s,
    x_r,
    cal_s,
    cal_r,
    d2d_s,
    d2d_r,
    ex_s,
    ex_r,
    own_sem,
):
    z, y, x, c = (lax.axis_index(name) for name in ("z", "y", "x", "c"))
    zp, zm, zo = (z + 1) % 4, (z + 3) % 4, (z + 2) % 4
    xp, xm, xo = (x + 1) % 4, (x + 3) % 4, (x + 2) % 4
    y2 = y % 2
    yq = y + 1 - 2 * y2
    sib = 1 - c
    me_t = z * 4 + y

    def piece(zz, row, half):
        return calbuf.at[c, zz * 2 + row, pl.ds(half * HALF, HALF), :]

    def own_piece(half):
        return cal_ref.at[pl.ds(half * HALF, HALF), :]

    def cal_copy(src, dst, sem, device):
        return pltpu.make_async_remote_copy(
            src_ref=src,
            dst_ref=dst,
            send_sem=cal_s.at[sem],
            recv_sem=cal_r.at[sem],
            device_id=device,
            device_id_type=MESH,
        )

    up, down, across = (zp, y, x, c), (zm, y, x, c), (z, yq, x, c)

    def send_up(k):
        src = (
            own_piece(0),
            own_piece(1),
            piece(zm, y2, 0),
            piece(z, 1 - y2, 0),
            piece(zm, 1 - y2, 0),
        )[k]
        dst = (
            piece(z, y2, 0),
            piece(z, y2, 1),
            piece(zm, y2, 0),
            piece(z, 1 - y2, 0),
            piece(zm, 1 - y2, 0),
        )[k]
        return cal_copy(src, dst, k, up)

    def send_down(k):
        src = (
            own_piece(1),
            own_piece(0),
            piece(zp, y2, 1),
            piece(z, 1 - y2, 1),
            piece(zp, 1 - y2, 1),
        )[k]
        dst = (
            piece(z, y2, 1),
            piece(z, y2, 0),
            piece(zp, y2, 1),
            piece(z, 1 - y2, 1),
            piece(zp, 1 - y2, 1),
        )[k]
        return cal_copy(src, dst, 5 + k, down)

    def send_across(k):
        src = (own_piece(0), own_piece(1), piece(zm, y2, 1), piece(zp, y2, 0))[k]
        dst = (piece(z, y2, 0), piece(z, y2, 1), piece(zm, y2, 1), piece(zp, y2, 0))[k]
        return cal_copy(src, dst, 10 + k, across)

    from_below = (
        (zm, y2, 0),
        (zm, y2, 1),
        (zo, y2, 0),
        (zm, 1 - y2, 0),
        (zo, 1 - y2, 0),
    )
    from_above = (
        (zp, y2, 1),
        (zp, y2, 0),
        (zo, y2, 1),
        (zp, 1 - y2, 1),
        (zo, 1 - y2, 1),
    )
    from_across = ((z, 1 - y2, 0), (z, 1 - y2, 1), (zm, 1 - y2, 1), (zp, 1 - y2, 0))

    def share(src, zz, row, half):
        at = (zz * 2 + row) * 2 + half
        return pltpu.make_async_remote_copy(
            src_ref=src,
            dst_ref=piece(zz, row, half),
            send_sem=d2d_s.at[at],
            recv_sem=d2d_r.at[at],
            device_id=(z, y, x, sib),
            device_id_type=MESH,
        )

    def arrive(sem, where, device):
        spot = piece(*where)
        cal_copy(spot, spot, sem, device).wait_recv()
        share(spot, *where).start()

    def arrive_below(k):
        arrive(k, from_below[k], down)

    def arrive_above(k):
        arrive(5 + k, from_above[k], up)

    def arrive_across(k):
        arrive(10 + k, from_across[k], across)

    own_copy = pltpu.make_async_copy(cal_ref, calbuf.at[c, z * 2 + y2], own_sem)

    barrier = pltpu.get_barrier_semaphore()

    def greet(device):
        pl.semaphore_signal(barrier, inc=1, device_id=device, device_id_type=MESH)

    home = y // 2
    for device in (up, down, across, (z, y, x, sib), (z, 3 - y, x, 1)):
        greet(device)
    for device in ((z, y, xp, c), (z, y, xm, c)):
        greet(device)

    @pl.loop(0, OWNERS)
    def _(t):
        zs, ys = t // 4, t % 4

        @pl.when(jnp.logical_not((zs == z) & (ys == y) & (home == c)))
        def _():
            greet((zs, ys, x, home))

    homed = home * c + (1 - home) * (1 - c)
    pl.semaphore_wait(barrier, OWNERS + 6 + 2 * c - homed)

    send_up(0).start()
    send_down(0).start()
    send_across(0).start()
    own_copy.start()

    live = lax.broadcasted_iota(jnp.int32, (1, BLOCKS), 1) < count_ref[...]
    owner_row = jnp.where(live, owner_ref[...], -1)
    mask = owner_row == lax.broadcasted_iota(jnp.int32, (OWNERS, BLOCKS), 0)
    maskf = mask.astype(F32)
    steps = BLOCKS // 128
    stack = jnp.concatenate(
        [maskf[:, j * 128 : (j + 1) * 128] for j in range(steps)], axis=0
    ).astype(BF16)
    row_id = lax.broadcasted_iota(jnp.int32, (128, 128), 0)
    col_id = lax.broadcasted_iota(jnp.int32, (128, 128), 1)
    strict = (row_id < col_id).astype(F32).astype(BF16)
    before = jnp.dot(stack, strict, preferred_element_type=F32)
    total = jnp.dot(stack, jnp.ones((128, 128), BF16), preferred_element_type=F32)
    offset = jnp.zeros((OWNERS, 128), F32)
    for j in range(steps):
        rank = before[j * OWNERS : (j + 1) * OWNERS] + offset
        ranks[:, j * 128 : (j + 1) * 128] = jnp.where(
            mask[:, j * 128 : (j + 1) * 128], rank.astype(jnp.int32), -1
        )
        offset = offset + total[j * OWNERS : (j + 1) * OWNERS]

    sensor = sensor_ref[...]
    kid = lax.broadcasted_iota(jnp.int32, (16, BLOCKS), 0)
    key_rows = jnp.where(
        kid == 0,
        sensor // 128,
        jnp.where(kid == 1, sensor % 128, jnp.where(kid == 2, window_ref[...], 0)),
    )
    payload[LENGTH:PAYLOAD, :] = key_rows.astype(F32).astype(BF16)

    lane = lax.broadcasted_iota(jnp.int32, (CHUNK, LENGTH), 1)

    @pl.loop(0, BLOCKS // CHUNK)
    def _(i):
        at = pl.ds(pl.multiple_of(i * CHUNK, CHUNK), CHUNK)
        samples = values_ref[at, :].astype(F32)
        offsets = shifts_ref[at, :].astype(F32)

        def product(k):
            weight = jnp.maximum(0.0, 1.0 - jnp.abs(offsets - k)).astype(BF16)
            return weight.astype(F32) * samples

        result = product(0.0)
        result = result + jnp.where(lane >= 1, pltpu.roll(product(1.0), 1, 1), 0.0)
        result = result + jnp.where(
            lane < LENGTH - 1, pltpu.roll(product(-1.0), LENGTH - 1, 1), 0.0
        )
        payload[0:LENGTH, at] = result.T.astype(BF16)

    def destination(k):
        zd = (z + k // 4) % 4
        cd = k % 2
        yd = 2 * c + (k // 2) % 2
        yo = yd + cd * (3 - 2 * yd)
        return zd, yd, cd, zd * 4 + yo

    def message_copy(k, zd, yd, cd):
        return pltpu.make_async_remote_copy(
            src_ref=outbuf.at[k],
            dst_ref=rx.at[x, me_t],
            send_sem=a2a_s.at[k],
            recv_sem=a2a_r.at[me_t],
            device_id=(zd, yd, x, cd),
            device_id_type=MESH,
        )

    low_lanes = lax.broadcasted_iota(jnp.int32, (1, 128), 1) < 64
    even = jnp.broadcast_to(y2, (1, 128)) == 0
    slot = lax.broadcasted_iota(jnp.int16, (256, BLOCKS), 0)
    slot = jnp.where(slot >= CAPACITY, slot - 64, slot)

    @pl.loop(0, OWNERS)
    def _(k):
        zd, yd, cd, owner = destination(k)
        rank = ranks[pl.ds(owner, 1), :].astype(jnp.int16)
        pick = jnp.where(rank == slot, jnp.ones((), BF16), jnp.zeros((), BF16))
        rows = lax.dot_general(payload[...], pick, NT, preferred_element_type=F32)
        outbuf[k, 0:PAYLOAD, :] = rows[:, 0:128].astype(BF16)
        top, bottom = rows[: PAYLOAD // 2, 128:256], rows[PAYLOAD // 2 :, 128:256]
        outbuf[k, PAYLOAD:MSG_ROWS, :] = jnp.where(
            low_lanes == even, top, bottom
        ).astype(BF16)
        is_self = (zd == z) & (yd == y) & (cd == c)

        @pl.when(jnp.logical_not(is_self))
        def _():
            message_copy(k, zd, yd, cd).start()

        @pl.when(is_self)
        def _():
            pltpu.make_async_copy(
                outbuf.at[k], rx.at[x, me_t], a2a_r.at[me_t]
            ).start()

    send_up(1).start()
    send_down(1).start()
    send_across(1).start()
    share(own_piece(0), z, y2, 0).start()
    share(own_piece(1), z, y2, 1).start()

    arrive_below(0)
    send_up(2).start()
    arrive_across(0)
    send_up(3).start()
    arrive_above(0)
    send_down(2).start()

    def x_copy(src_x, half, sem, device):
        span = rx.at[src_x, pl.ds(half * 8, 8)]
        return pltpu.make_async_remote_copy(
            src_ref=span,
            dst_ref=span,
            send_sem=x_s.at[sem],
            recv_sem=x_r.at[sem],
            device_id=device,
            device_id_type=MESH,
        )

    right, left = (z, y, xp, c), (z, y, xm, c)

    def message_wait(t):
        pltpu.make_async_copy(rx.at[x, t], rx.at[x, t], a2a_r.at[t]).wait()

    @pl.loop(0, 8)
    def _(t):
        message_wait(t)

    x_copy(x, 0, 0, right).start()

    @pl.loop(8, 16)
    def _(t):
        message_wait(t)

    x_copy(x, 1, 3, left).start()
    x_copy(x, 1, 1, right).start()
    x_copy(x, 0, 2, left).start()

    def place(q):
        @pl.loop(0, OWNERS // 2)
        def _(p):
            m0 = rx.at[q, 2 * p]
            m1 = rx.at[q, 2 * p + 1]
            r0 = m0[PAYLOAD:MSG_ROWS, :].astype(F32)
            r1 = m1[PAYLOAD:MSG_ROWS, :].astype(F32)
            upper = jnp.where(low_lanes, r0, r1)
            lower = pltpu.roll(jnp.where(low_lanes, r1, r0), 64, 1)
            joint = jnp.concatenate([upper, lower], axis=0)
            tiles = (
                m0[0:PAYLOAD, :].astype(F32),
                m1[0:PAYLOAD, :].astype(F32),
                joint,
            )
            for n, tile in enumerate(tiles):
                at = pl.ds(pl.multiple_of(p * 384 + n * 128, 128), 128)
                slot_sensor[0:1, at] = (
                    tile[LENGTH : LENGTH + 1] * 128.0 + tile[LENGTH + 1 : LENGTH + 2]
                ).astype(jnp.int32)
                window = tile[LENGTH + 2 : LENGTH + 3]
                for w in range(WINDOWS):
                    placed[w * 128 : (w + 1) * 128, at] = jnp.where(
                        window == float(w), tile[0:LENGTH], 0.0
                    ).astype(BF16)

        @pl.loop(0, GROUP // WIDE)
        def _(j):
            near = (slot_sensor[0:1, :] - j * WIDE).astype(jnp.int16)
            ids = lax.broadcasted_iota(jnp.int16, (WIDE, SLOTS), 0)
            hot[...] = jnp.where(ids == near, jnp.ones((), BF16), jnp.zeros((), BF16))
            block = lax.dot_general(placed[...], hot[...], NT, preferred_element_type=F32)
            at = pl.ds(pl.multiple_of(j * WIDE, WIDE), WIDE)
            aligned[q, :, at] = block.astype(BF16)

    place(x)

    arrive_below(1)
    arrive_above(1)
    send_across(2).start()
    send_across(3).start()
    arrive_across(1)
    send_down(3).start()

    x_copy(xm, 0, 0, left).wait_recv()
    x_copy(xm, 0, 4, right).start()
    x_copy(xp, 1, 3, right).wait_recv()
    x_copy(xp, 1, 5, left).start()
    x_copy(xm, 1, 1, left).wait_recv()
    place(xm)

    arrive_below(2)
    arrive_above(2)
    arrive_across(2)

    x_copy(xp, 0, 2, right).wait_recv()
    place(xp)

    arrive_below(3)
    send_up(4).start()
    arrive_above(3)
    send_down(4).start()
    arrive_across(3)

    x_copy(xo, 0, 4, left).wait_recv()
    x_copy(xo, 1, 5, right).wait_recv()
    place(xo)

    own_copy.wait()

    def shared(zz, row):
        for half in range(2):
            at = (zz * 2 + row) * 2 + half
            spot = calbuf.at[sib, zz * 2 + row, pl.ds(half * HALF, HALF), :]
            pltpu.make_async_remote_copy(
                src_ref=spot,
                dst_ref=spot,
                send_sem=d2d_s.at[at],
                recv_sem=d2d_r.at[at],
                device_id=(z, y, x, sib),
                device_id_type=MESH,
            ).wait_recv()

    acc[...] = jnp.zeros_like(acc)

    def multiply(zz):
        for panel in range(2):
            acc[panel] += jnp.dot(
                aligned[zz],
                calbuf[panel, pl.ds(zz * 2, 2)].reshape(GROUP, COLS),
                preferred_element_type=F32,
            )

    for zz in (z, zm, zp):
        shared(zz, 0)
        shared(zz, 1)
        multiply(zz)

    arrive_below(4)
    arrive_above(4)
    shared(zo, 0)
    shared(zo, 1)
    multiply(zo)

    give[...] = acc[...].astype(BF16)

    def exchange(panel, sem_s, sem_r, device):
        return pltpu.make_async_remote_copy(
            src_ref=give.at[panel],
            dst_ref=take.at[sem_r],
            send_sem=ex_s.at[sem_s],
            recv_sem=ex_r.at[sem_r],
            device_id=device,
            device_id_type=MESH,
        )

    @pl.when(c == 0)
    def _():
        over = exchange(1, 0, 0, (z, y, x, 1))
        over.start()
        exchange(0, 0, 0, (z, 3 - y, x, 1)).wait_recv()
        out_ref[...] = (acc[0] + take[0].astype(F32)).astype(BF16)
        over.wait_send()

    @pl.when(c == 1)
    def _():
        first = exchange(0, 0, 0, (z, 3 - y, x, 0))
        first.start()
        second = exchange(1, 1, 1, (z, 3 - y, x, 1))
        second.start()
        exchange(0, 0, 0, (z, y, x, 0)).wait_recv()
        exchange(1, 1, 1, (z, 3 - y, x, 1)).wait_recv()
        out_ref[...] = (take[0].astype(F32) + take[1].astype(F32)).astype(BF16)
        first.wait_send()
        second.wait_send()

    for k in range(5):
        send_up(k).wait_send()
        send_down(k).wait_send()
    for k in range(4):
        send_across(k).wait_send()
    share(own_piece(0), z, y2, 0).wait_send()
    share(own_piece(1), z, y2, 1).wait_send()
    for where in from_below + from_above + from_across:
        share(piece(*where), *where).wait_send()
    x_copy(x, 0, 0, right).wait_send()
    x_copy(x, 1, 1, right).wait_send()
    x_copy(x, 0, 2, left).wait_send()
    x_copy(x, 1, 3, left).wait_send()
    x_copy(xm, 0, 4, right).wait_send()
    x_copy(xp, 1, 5, left).wait_send()

    @pl.loop(0, OWNERS)
    def _(k):
        zd, yd, cd, _owner = destination(k)

        @pl.when(jnp.logical_not((zd == z) & (yd == y) & (cd == c)))
        def _():
            message_copy(k, zd, yd, cd).wait_send()


def per_device(
    block_values, block_shifts, block_sensor, block_window, block_owner, block_counts, calibration
):
    vmem = pl.BlockSpec(memory_space=pltpu.VMEM)
    return pl.pallas_call(
        kernel,
        out_shape=jax.ShapeDtypeStruct((ROWS, COLS), BF16),
        in_specs=[vmem] * 6 + [pl.BlockSpec(memory_space=pl.ANY)],
        out_specs=vmem,
        scratch_shapes=[
            pltpu.VMEM((OWNERS, BLOCKS), jnp.int32),
            pltpu.VMEM((PAYLOAD, BLOCKS), BF16),
            pltpu.VMEM((OWNERS, MSG_ROWS, LENGTH), BF16),
            pltpu.VMEM((4, OWNERS, MSG_ROWS, LENGTH), BF16),
            pltpu.VMEM((ROWS, SLOTS), BF16),
            pltpu.VMEM((8, SLOTS), jnp.int32),
            pltpu.VMEM((WIDE, SLOTS), BF16),
            pltpu.VMEM((4, ROWS, GROUP), BF16),
            pltpu.VMEM((2, 8, CAL_ROWS, COLS), BF16),
            pltpu.VMEM((2, ROWS, COLS), F32),
            pltpu.VMEM((2, ROWS, COLS), BF16),
            pltpu.VMEM((2, ROWS, COLS), BF16),
            pltpu.SemaphoreType.DMA((OWNERS,)),
            pltpu.SemaphoreType.DMA((OWNERS,)),
            pltpu.SemaphoreType.DMA((6,)),
            pltpu.SemaphoreType.DMA((6,)),
            pltpu.SemaphoreType.DMA((14,)),
            pltpu.SemaphoreType.DMA((14,)),
            pltpu.SemaphoreType.DMA((16,)),
            pltpu.SemaphoreType.DMA((16,)),
            pltpu.SemaphoreType.DMA((2,)),
            pltpu.SemaphoreType.DMA((2,)),
            pltpu.SemaphoreType.DMA,
        ],
        compiler_params=pltpu.CompilerParams(
            collective_id=0, has_side_effects=True, vmem_limit_bytes=60 * 1024 * 1024
        ),
    )(
        block_values[0],
        block_shifts[0],
        block_sensor,
        block_window,
        block_owner.reshape(1, BLOCKS),
        block_counts,
        calibration,
    )


def solution(mesh):
    torus = Mesh(mesh.devices.reshape(4, 4, 4, 2), ("z", "y", "x", "c"))
    tm, col = ("z", "y"), ("x", "c")
    in_specs = (
        P(col, tm, None),
        P(col, tm, None),
        P(col, tm),
        P(col, tm),
        P(col, tm, None),
        P(col, tm),
        P(tm, col),
    )
    return jax.shard_map(
        per_device, mesh=torus, in_specs=in_specs, out_specs=P(tm, col), check_vma=False
    )
```

```python
import jax
import jax.numpy as jnp
from jax import lax
from jax.experimental import pallas as pl
from jax.experimental.pallas import tpu as pltpu
from jax.sharding import Mesh
from jax.sharding import PartitionSpec as P

MESH = pl.DeviceIdType.MESH
F32 = jnp.float32
BF16 = jnp.bfloat16

LENGTH = 128
BLOCKS = 2048
OWNERS = 16
CAPACITY = 192
WINDOWS = 4
GROUP = 2048
ROWS = 512
COLS = 512
CAL_ROWS = 1024
HALF = CAL_ROWS // 2
PARTS = 2
PART = COLS // PARTS
DEPTH = 4 * GROUP
PAYLOAD = LENGTH + 16
MSG_ROWS = PAYLOAD + PAYLOAD // 2
SLOTS = OWNERS * CAPACITY
CHUNK = 256
WIDE = 1024
NT = (((1,), (1,)), ((), ()))


def kernel(
    values_ref,
    shifts_ref,
    sensor_ref,
    window_ref,
    owner_ref,
    count_ref,
    cal_ref,
    out_ref,
    ranks,
    payload,
    outbuf,
    rx,
    placed,
    slot_sensor,
    hot,
    aligned,
    calbuf,
    acc,
    mine,
    give,
    take,
    a2a_s,
    a2a_r,
    x_s,
    x_r,
    cal_s,
    cal_r,
    d2d_s,
    d2d_r,
    ex_s,
    ex_r,
    own_sem,
):
    z, y, x, c = (lax.axis_index(name) for name in ("z", "y", "x", "c"))
    zp, zm, zo = (z + 1) % 4, (z + 3) % 4, (z + 2) % 4
    xp, xm, xo = (x + 1) % 4, (x + 3) % 4, (x + 2) % 4
    y2 = y % 2
    yq = y + 1 - 2 * y2
    sib = 1 - c
    me_t = z * 4 + y

    def lanes(core):
        return pl.ds(pl.multiple_of(core * PART, PART), PART)

    def piece(n, zz, row, half):
        at = pl.ds((zz * 2 + row) * CAL_ROWS + half * HALF, HALF)
        return calbuf.at[n, at, lanes(c)]

    def own_piece(n, half):
        return cal_ref.at[pl.ds(half * HALF, HALF), pl.ds(n * PART, PART)]

    def cal_copy(n, src, dst, sem, device):
        return pltpu.make_async_remote_copy(
            src_ref=src,
            dst_ref=dst,
            send_sem=cal_s.at[n * 14 + sem],
            recv_sem=cal_r.at[n * 14 + sem],
            device_id=device,
            device_id_type=MESH,
        )

    up, down, across = (zp, y, x, c), (zm, y, x, c), (z, yq, x, c)

    def relay(n, sem, spot, device):
        own = spot[0] is z and spot[1] is y2
        src = own_piece(n, spot[2]) if own else piece(n, *spot)
        return cal_copy(n, src, piece(n, *spot), sem, device)

    other = 1 - y2
    go_up = ((z, y2, 0), (z, y2, 1), (zm, y2, 0), (z, other, 0), (zm, other, 0))
    go_down = ((z, y2, 1), (z, y2, 0), (zp, y2, 1), (z, other, 1), (zp, other, 1))
    go_across = ((z, y2, 0), (z, y2, 1), (zm, y2, 1), (zp, y2, 0))

    def send_up(n, k):
        return relay(n, k, go_up[k], up)

    def send_down(n, k):
        return relay(n, 5 + k, go_down[k], down)

    def send_across(n, k):
        return relay(n, 10 + k, go_across[k], across)

    from_below = ((zm, y2, 0), (zm, y2, 1), (zo, y2, 0), (zm, other, 0), (zo, other, 0))
    from_above = ((zp, y2, 1), (zp, y2, 0), (zo, y2, 1), (zp, other, 1), (zo, other, 1))
    from_across = ((z, other, 0), (z, other, 1), (zm, other, 1), (zp, other, 0))

    def share(n, src, zz, row, half):
        at = n * 16 + (zz * 2 + row) * 2 + half
        return pltpu.make_async_remote_copy(
            src_ref=src,
            dst_ref=piece(n, zz, row, half),
            send_sem=d2d_s.at[at],
            recv_sem=d2d_r.at[at],
            device_id=(z, y, x, sib),
            device_id_type=MESH,
        )

    def arrive(n, sem, where, device):
        spot = piece(n, *where)
        cal_copy(n, spot, spot, sem, device).wait_recv()
        share(n, spot, *where).start()

    def below(n, k):
        arrive(n, k, from_below[k], down)

    def above(n, k):
        arrive(n, 5 + k, from_above[k], up)

    def beside(n, k):
        arrive(n, 10 + k, from_across[k], across)

    def own_copy(n):
        at = pl.ds((z * 2 + y2) * CAL_ROWS, CAL_ROWS)
        return pltpu.make_async_copy(
            cal_ref.at[:, pl.ds(n * PART, PART)], calbuf.at[n, at, lanes(c)], own_sem.at[n]
        )


    barrier = pltpu.get_barrier_semaphore()

    def greet(device):
        pl.semaphore_signal(barrier, inc=1, device_id=device, device_id_type=MESH)

    home = y // 2
    for device in (up, down, across, (z, y, x, sib), (z, 3 - y, x, 1)):
        greet(device)
    for device in ((z, y, xp, c), (z, y, xm, c)):
        greet(device)

    @pl.loop(0, OWNERS)
    def _(t):
        zs, ys = t // 4, t % 4

        @pl.when(jnp.logical_not((zs == z) & (ys == y) & (home == c)))
        def _():
            greet((zs, ys, x, home))

    homed = home * c + (1 - home) * (1 - c)
    pl.semaphore_wait(barrier, OWNERS + 6 + 2 * c - homed)

    def first(n):
        send_up(n, 0).start()
        send_down(n, 0).start()
        send_across(n, 0).start()

    def second(n):
        send_up(n, 1).start()
        send_down(n, 1).start()
        send_across(n, 1).start()

    def share_own(n):
        own_copy(n).start()
        for half in range(2):
            share(n, own_piece(n, half), z, y2, half).start()

    first(0)

    live = lax.broadcasted_iota(jnp.int32, (1, BLOCKS), 1) < count_ref[...]
    owner_row = jnp.where(live, owner_ref[...], -1)
    mask = owner_row == lax.broadcasted_iota(jnp.int32, (OWNERS, BLOCKS), 0)
    maskf = mask.astype(F32)
    steps = BLOCKS // 128
    stack = jnp.concatenate(
        [maskf[:, j * 128 : (j + 1) * 128] for j in range(steps)], axis=0
    ).astype(BF16)
    row_id = lax.broadcasted_iota(jnp.int32, (128, 128), 0)
    col_id = lax.broadcasted_iota(jnp.int32, (128, 128), 1)
    strict = (row_id < col_id).astype(F32).astype(BF16)
    before = jnp.dot(stack, strict, preferred_element_type=F32)
    total = jnp.dot(stack, jnp.ones((128, 128), BF16), preferred_element_type=F32)
    offset = jnp.zeros((OWNERS, 128), F32)
    for j in range(steps):
        rank = before[j * OWNERS : (j + 1) * OWNERS] + offset
        ranks[:, j * 128 : (j + 1) * 128] = jnp.where(
            mask[:, j * 128 : (j + 1) * 128], rank.astype(jnp.int32), -1
        )
        offset = offset + total[j * OWNERS : (j + 1) * OWNERS]

    sensor = sensor_ref[...]
    kid = lax.broadcasted_iota(jnp.int32, (16, BLOCKS), 0)
    key_rows = jnp.where(
        kid == 0,
        sensor // 128,
        jnp.where(kid == 1, sensor % 128, jnp.where(kid == 2, window_ref[...], 0)),
    )
    payload[LENGTH:PAYLOAD, :] = key_rows.astype(F32).astype(BF16)

    lane = lax.broadcasted_iota(jnp.int32, (CHUNK, LENGTH), 1)

    @pl.loop(0, BLOCKS // CHUNK)
    def _(i):
        at = pl.ds(pl.multiple_of(i * CHUNK, CHUNK), CHUNK)
        samples = values_ref[at, :].astype(F32)
        offsets = shifts_ref[at, :].astype(F32)

        def product(k):
            weight = jnp.maximum(0.0, 1.0 - jnp.abs(offsets - k)).astype(BF16)
            return weight.astype(F32) * samples

        result = product(0.0)
        result = result + jnp.where(lane >= 1, pltpu.roll(product(1.0), 1, 1), 0.0)
        result = result + jnp.where(
            lane < LENGTH - 1, pltpu.roll(product(-1.0), LENGTH - 1, 1), 0.0
        )
        payload[0:LENGTH, at] = result.T.astype(BF16)

    def destination(k):
        zd = (z + k // 4) % 4
        cd = k % 2
        yd = 2 * c + (k // 2) % 2
        yo = yd + cd * (3 - 2 * yd)
        return zd, yd, cd, zd * 4 + yo

    def message_copy(k, zd, yd, cd):
        return pltpu.make_async_remote_copy(
            src_ref=outbuf.at[k],
            dst_ref=rx.at[x, me_t],
            send_sem=a2a_s.at[k],
            recv_sem=a2a_r.at[me_t],
            device_id=(zd, yd, x, cd),
            device_id_type=MESH,
        )

    low_lanes = lax.broadcasted_iota(jnp.int32, (1, 128), 1) < 64
    even = jnp.broadcast_to(y2, (1, 128)) == 0
    lead_slot = lax.broadcasted_iota(jnp.int16, (128, BLOCKS), 0)
    tail_slot = lax.broadcasted_iota(jnp.int16, (64, BLOCKS), 0) + 128
    fold = PAYLOAD // 2

    def hit(owner, slot):
        rank = ranks[pl.ds(owner, 1), :].astype(jnp.int16)
        return jnp.where(rank == slot, jnp.ones((), BF16), jnp.zeros((), BF16))

    def send_message(k):
        zd, yd, cd, _owner = destination(k)
        is_self = (zd == z) & (yd == y) & (cd == c)

        @pl.when(jnp.logical_not(is_self))
        def _():
            message_copy(k, zd, yd, cd).start()

        @pl.when(is_self)
        def _():
            pltpu.make_async_copy(
                outbuf.at[k], rx.at[x, me_t], a2a_r.at[me_t]
            ).start()

    def messages(start, stop):
        @pl.loop(start, stop)
        def _(pair):
            k0, k1 = 2 * pair, 2 * pair + 1
            owner0, owner1 = destination(k0)[3], destination(k1)[3]
            pick = jnp.concatenate(
                [
                    hit(owner0, lead_slot),
                    hit(owner1, lead_slot),
                    hit(owner0, tail_slot),
                    hit(owner1, tail_slot),
                ],
                axis=0,
            )
            rows = lax.dot_general(payload[...], pick, NT, preferred_element_type=F32)
            outbuf[k0, 0:PAYLOAD, :] = rows[:, 0:128].astype(BF16)
            outbuf[k1, 0:PAYLOAD, :] = rows[:, 128:256].astype(BF16)
            tail = rows[:, 256:384]
            swapped = pltpu.roll(tail, 64, 1)
            near0 = jnp.where(even, tail[:fold], tail[fold:])
            far0 = jnp.where(even, swapped[fold:], swapped[:fold])
            near1 = jnp.where(even, swapped[:fold], swapped[fold:])
            far1 = jnp.where(even, tail[fold:], tail[:fold])
            outbuf[k0, PAYLOAD:MSG_ROWS, :] = jnp.where(low_lanes, near0, far0).astype(BF16)
            outbuf[k1, PAYLOAD:MSG_ROWS, :] = jnp.where(low_lanes, near1, far1).astype(BF16)
            send_message(k0)
            send_message(k1)

    def x_copy(src_x, group, sem, device):
        span = rx.at[src_x, pl.ds((z + 4 - group) % 4 * 4, 4)]
        return pltpu.make_async_remote_copy(
            src_ref=span,
            dst_ref=span,
            send_sem=x_s.at[sem],
            recv_sem=x_r.at[sem],
            device_id=device,
            device_id_type=MESH,
        )

    right, left = (z, y, xp, c), (z, y, xm, c)

    def spread(group):
        @pl.loop(0, 4)
        def _(i):
            t = (z + 4 - group) % 4 * 4 + i
            pltpu.make_async_copy(rx.at[x, t], rx.at[x, t], a2a_r.at[t]).wait()

        x_copy(x, group, group, right).start()
        x_copy(x, group, 4 + group, left).start()

    messages(0, 8)
    share_own(0)
    second(0)
    for group in range(4):
        spread(group)

    below(0, 0)
    beside(0, 0)
    above(0, 0)
    send_up(0, 2).start()
    send_down(0, 2).start()
    send_up(0, 3).start()
    first(1)
    share_own(1)
    acc[...] = jnp.zeros_like(acc)

    def prepare(q):
        @pl.loop(0, OWNERS // 2)
        def _(p):
            m0 = rx.at[q, 2 * p]
            m1 = rx.at[q, 2 * p + 1]
            r0 = m0[PAYLOAD:MSG_ROWS, :].astype(F32)
            r1 = m1[PAYLOAD:MSG_ROWS, :].astype(F32)
            upper = jnp.where(low_lanes, r0, r1)
            lower = pltpu.roll(jnp.where(low_lanes, r1, r0), 64, 1)
            joint = jnp.concatenate([upper, lower], axis=0)
            tiles = (
                m0[0:PAYLOAD, :].astype(F32),
                m1[0:PAYLOAD, :].astype(F32),
                joint,
            )
            for n, tile in enumerate(tiles):
                at = pl.ds(pl.multiple_of(p * 384 + n * 128, 128), 128)
                slot_sensor[0:1, at] = (
                    tile[LENGTH : LENGTH + 1] * 128.0 + tile[LENGTH + 1 : LENGTH + 2]
                ).astype(jnp.int32)
                window = tile[LENGTH + 2 : LENGTH + 3]
                for w in range(WINDOWS):
                    placed[w * 128 : (w + 1) * 128, at] = jnp.where(
                        window == float(w), tile[0:LENGTH], 0.0
                    ).astype(BF16)

    def place(q, j):
        near = (slot_sensor[0:1, :] - j * WIDE).astype(jnp.int16)
        ids = lax.broadcasted_iota(jnp.int16, (WIDE, SLOTS), 0)
        hot[...] = jnp.where(ids == near, jnp.ones((), BF16), jnp.zeros((), BF16))
        block = lax.dot_general(placed[...], hot[...], NT, preferred_element_type=F32)
        at = pl.ds(pl.multiple_of(q * GROUP + j * WIDE, WIDE), WIDE)
        aligned[:, at] = block.astype(BF16)

    def shared(n, zz):
        @pl.loop(0, 4)
        def _(i):
            at = n * 16 + zz * 4 + i
            spot = calbuf.at[n, pl.ds(zz * GROUP + i * HALF, HALF), lanes(sib)]
            pltpu.make_async_remote_copy(
                src_ref=spot,
                dst_ref=spot,
                send_sem=d2d_s.at[at],
                recv_sem=d2d_r.at[at],
                device_id=(z, y, x, sib),
                device_id_type=MESH,
            ).wait_recv()

    def multiply(n, zz):
        depth = pl.ds(pl.multiple_of(zz * GROUP, GROUP), GROUP)
        return jnp.dot(
            aligned[:, depth], calbuf[n, depth, :], preferred_element_type=F32
        )

    def early(n):
        own_copy(n).wait()
        for zz in (z, zm, zp):
            shared(n, zz)

        @pl.loop(0, 3)
        def _(i):
            acc[n] += multiply(n, (z + 3 * i - i // 2) % 4)

    def exchange(n, panel, sem_s, sem_r, device):
        return pltpu.make_async_remote_copy(
            src_ref=give.at[panel, n],
            dst_ref=take.at[sem_r, n],
            send_sem=ex_s.at[n * 2 + sem_s],
            recv_sem=ex_r.at[n * 2 + sem_r],
            device_id=device,
            device_id_type=MESH,
        )

    def late(n):
        shared(n, zo)
        total = acc[n] + multiply(n, zo)
        for panel in range(2):
            give[panel, n] = total[:, panel * PART : (panel + 1) * PART].astype(BF16)
        mine[n] = total[:, :PART]

        @pl.when(c == 0)
        def _():
            exchange(n, 1, 0, 0, (z, y, x, 1)).start()

        @pl.when(c == 1)
        def _():
            exchange(n, 0, 0, 0, (z, 3 - y, x, 0)).start()
            exchange(n, 1, 1, 1, (z, 3 - y, x, 1)).start()

    def finish(n):
        at = slice(n * PART, (n + 1) * PART)

        @pl.when(c == 0)
        def _():
            exchange(n, 0, 0, 0, (z, 3 - y, x, 1)).wait_recv()
            out_ref[:, at] = (mine[n] + take[0, n].astype(F32)).astype(BF16)
            exchange(n, 1, 0, 0, (z, y, x, 1)).wait_send()

        @pl.when(c == 1)
        def _():
            exchange(n, 0, 0, 0, (z, y, x, 0)).wait_recv()
            exchange(n, 1, 1, 1, (z, 3 - y, x, 1)).wait_recv()
            out_ref[:, at] = (take[0, n].astype(F32) + take[1, n].astype(F32)).astype(BF16)
            exchange(n, 0, 0, 0, (z, 3 - y, x, 0)).wait_send()
            exchange(n, 1, 1, 1, (z, 3 - y, x, 1)).wait_send()

    prepare(x)
    place(x, 0)
    beside(0, 1)
    send_down(0, 3).start()
    send_across(1, 1).start()
    place(x, 1)

    below(0, 1)
    above(0, 1)
    send_across(0, 2).start()
    send_across(0, 3).start()
    send_down(1, 1).start()
    send_up(1, 1).start()

    for group in range(2):
        x_copy(xm, group, group, left).wait_recv()
        x_copy(xm, group, 8 + group, right).start()
    for group in range(2, 4):
        x_copy(xp, group, 4 + group, right).wait_recv()
        x_copy(xp, group, 8 + group, left).start()
    x_copy(xm, 2, 2, left).wait_recv()
    x_copy(xm, 3, 3, left).wait_recv()

    prepare(xm)
    place(xm, 0)
    below(0, 3)
    send_up(0, 4).start()
    beside(1, 0)
    send_up(1, 3).start()
    beside(1, 1)
    send_down(1, 3).start()
    place(xm, 1)

    below(0, 2)
    above(0, 2)
    above(0, 3)
    send_down(0, 4).start()
    below(1, 0)
    send_up(1, 2).start()
    above(1, 0)
    send_down(1, 2).start()

    x_copy(xp, 0, 4, right).wait_recv()
    x_copy(xp, 1, 5, right).wait_recv()
    prepare(xp)
    place(xp, 0)
    below(1, 1)
    above(1, 1)
    send_across(1, 2).start()
    send_across(1, 3).start()
    beside(0, 2)
    beside(0, 3)
    place(xp, 1)

    x_copy(xo, 0, 8, left).wait_recv()
    x_copy(xo, 1, 9, left).wait_recv()
    x_copy(xo, 2, 10, right).wait_recv()
    x_copy(xo, 3, 11, right).wait_recv()
    prepare(xo)
    place(xo, 0)
    below(1, 3)
    send_up(1, 4).start()
    above(1, 3)
    send_down(1, 4).start()
    place(xo, 1)

    below(0, 4)
    above(0, 4)
    early(0)
    late(0)

    beside(1, 2)
    beside(1, 3)
    below(1, 2)
    above(1, 2)
    early(1)
    below(1, 4)
    above(1, 4)
    late(1)
    finish(0)
    finish(1)

    for n in range(PARTS):
        for k in range(5):
            send_up(n, k).wait_send()
            send_down(n, k).wait_send()
        for k in range(4):
            send_across(n, k).wait_send()

        @pl.loop(0, 16)
        def _(at):
            spot = calbuf.at[n, pl.ds(at * HALF, HALF), lanes(c)]
            pltpu.make_async_remote_copy(
                src_ref=spot,
                dst_ref=spot,
                send_sem=d2d_s.at[n * 16 + at],
                recv_sem=d2d_r.at[n * 16 + at],
                device_id=(z, y, x, sib),
                device_id_type=MESH,
            ).wait_send()

    for group in range(4):
        x_copy(x, group, group, right).wait_send()
        x_copy(x, group, 4 + group, left).wait_send()
    for group in range(2):
        x_copy(xm, group, 8 + group, right).wait_send()
        x_copy(xp, 2 + group, 10 + group, left).wait_send()

    @pl.loop(0, OWNERS)
    def _(k):
        zd, yd, cd, _owner = destination(k)

        @pl.when(jnp.logical_not((zd == z) & (yd == y) & (cd == c)))
        def _():
            message_copy(k, zd, yd, cd).wait_send()


def per_device(
    block_values, block_shifts, block_sensor, block_window, block_owner, block_counts, calibration
):
    vmem = pl.BlockSpec(memory_space=pltpu.VMEM)
    return pl.pallas_call(
        kernel,
        out_shape=jax.ShapeDtypeStruct((ROWS, COLS), BF16),
        in_specs=[vmem] * 6 + [pl.BlockSpec(memory_space=pl.ANY)],
        out_specs=vmem,
        scratch_shapes=[
            pltpu.VMEM((OWNERS, BLOCKS), jnp.int32),
            pltpu.VMEM((PAYLOAD, BLOCKS), BF16),
            pltpu.VMEM((OWNERS, MSG_ROWS, LENGTH), BF16),
            pltpu.VMEM((4, OWNERS, MSG_ROWS, LENGTH), BF16),
            pltpu.VMEM((ROWS, SLOTS), BF16),
            pltpu.VMEM((8, SLOTS), jnp.int32),
            pltpu.VMEM((WIDE, SLOTS), BF16),
            pltpu.VMEM((ROWS, DEPTH), BF16),
            pltpu.VMEM((PARTS, DEPTH, 2 * PART), BF16),
            pltpu.VMEM((PARTS, ROWS, 2 * PART), F32),
            pltpu.VMEM((PARTS, ROWS, PART), F32),
            pltpu.VMEM((2, PARTS, ROWS, PART), BF16),
            pltpu.VMEM((2, PARTS, ROWS, PART), BF16),
            pltpu.SemaphoreType.DMA((OWNERS,)),
            pltpu.SemaphoreType.DMA((OWNERS,)),
            pltpu.SemaphoreType.DMA((12,)),
            pltpu.SemaphoreType.DMA((12,)),
            pltpu.SemaphoreType.DMA((PARTS * 14,)),
            pltpu.SemaphoreType.DMA((PARTS * 14,)),
            pltpu.SemaphoreType.DMA((PARTS * 16,)),
            pltpu.SemaphoreType.DMA((PARTS * 16,)),
            pltpu.SemaphoreType.DMA((PARTS * 2,)),
            pltpu.SemaphoreType.DMA((PARTS * 2,)),
            pltpu.SemaphoreType.DMA((PARTS,)),
        ],
        compiler_params=pltpu.CompilerParams(
            collective_id=0, has_side_effects=True, vmem_limit_bytes=60 * 1024 * 1024
        ),
    )(
        block_values[0],
        block_shifts[0],
        block_sensor,
        block_window,
        block_owner.reshape(1, BLOCKS),
        block_counts,
        calibration,
    )


def solution(mesh):
    torus = Mesh(mesh.devices.reshape(4, 4, 4, 2), ("z", "y", "x", "c"))
    tm, col = ("z", "y"), ("x", "c")
    in_specs = (
        P(col, tm, None),
        P(col, tm, None),
        P(col, tm),
        P(col, tm),
        P(col, tm, None),
        P(col, tm),
        P(tm, col),
    )
    return jax.shard_map(
        per_device, mesh=torus, in_specs=in_specs, out_specs=P(tm, col), check_vma=False
    )
```

```python
import jax
import jax.numpy as jnp
from jax import lax
from jax.experimental import pallas as pl
from jax.experimental.pallas import tpu as pltpu
from jax.sharding import Mesh
from jax.sharding import PartitionSpec as P

MESH = pl.DeviceIdType.MESH
F32 = jnp.float32
BF16 = jnp.bfloat16

LENGTH = 128
BLOCKS = 2048
OWNERS = 16
CAPACITY = 192
WINDOWS = 4
GROUP = 2048
ROWS = 512
COLS = 512
CAL_ROWS = 1024
HALF = CAL_ROWS // 2
WIDTHS = (128, 128, 128, 128)
PARTS = len(WIDTHS)
STARTS = tuple(sum(WIDTHS[:n]) for n in range(PARTS))
MOVES = 16
EASED = (2,)
DEPTH = 4 * GROUP
PAYLOAD = LENGTH + 16
MSG_ROWS = PAYLOAD + PAYLOAD // 2
SLOTS = OWNERS * CAPACITY
CHUNK = 256
WIDE = 1024
NT = (((1,), (1,)), ((), ()))


def kernel(
    values_ref,
    shifts_ref,
    sensor_ref,
    window_ref,
    owner_ref,
    count_ref,
    cal_ref,
    out_ref,
    ranks,
    payload,
    outbuf,
    rx,
    placed,
    slot_sensor,
    hot,
    aligned,
    calbuf,
    acc,
    mine,
    give,
    take,
    done,
    a2a_s,
    a2a_r,
    x_s,
    x_r,
    cal_s,
    cal_r,
    d2d_s,
    d2d_r,
    ex_s,
    ex_r,
    own_sem,
    out_sem,
):
    z, y, x, c = (lax.axis_index(name) for name in ("z", "y", "x", "c"))
    zp, zm, zo = (z + 1) % 4, (z + 3) % 4, (z + 2) % 4
    xp, xm, xo = (x + 1) % 4, (x + 3) % 4, (x + 2) % 4
    y2 = y % 2
    yq = y + 1 - 2 * y2
    sib = 1 - c
    me_t = z * 4 + y

    def lanes(n, core):
        at = 2 * STARTS[n] + core * WIDTHS[n]
        return pl.ds(pl.multiple_of(at, 128), WIDTHS[n])

    def both(n):
        return slice(2 * STARTS[n], 2 * STARTS[n] + 2 * WIDTHS[n])

    def piece(n, zz, row, half):
        at = pl.ds((zz * 2 + row) * CAL_ROWS + half * HALF, HALF)
        return calbuf.at[at, lanes(n, c)]

    def own_piece(n, half):
        return cal_ref.at[pl.ds(half * HALF, HALF), pl.ds(STARTS[n], WIDTHS[n])]

    def cal_copy(n, src, dst, sem, device):
        return pltpu.make_async_remote_copy(
            src_ref=src,
            dst_ref=dst,
            send_sem=cal_s.at[n],
            recv_sem=cal_r.at[n * MOVES + sem],
            device_id=device,
            device_id_type=MESH,
        )

    up, down, across = (zp, y, x, c), (zm, y, x, c), (z, yq, x, c)

    def relay(n, sem, spot, device):
        own = spot[0] is z and spot[1] is y2
        src = own_piece(n, spot[2]) if own else piece(n, *spot)
        return cal_copy(n, src, piece(n, *spot), sem, device)

    other = 1 - y2
    go_up = ((z, y2, 0), (z, y2, 1), (zm, y2, 0), (z, other, 0), (zm, other, 0))
    go_down = ((z, y2, 1), (z, y2, 0), (zp, y2, 1), (z, other, 1), (zp, other, 1))
    go_across = (
        (z, y2, 0),
        (z, y2, 1),
        (zm, y2, 1),
        (zp, y2, 0),
        (zm, y2, 0),
        (zp, y2, 1),
    )

    def send_up(n, k):
        return relay(n, k, go_up[k], up)

    def send_down(n, k):
        return relay(n, 5 + k, go_down[k], down)

    def send_across(n, k):
        return relay(n, 10 + k, go_across[k], across)

    from_below = ((zm, y2, 0), (zm, y2, 1), (zo, y2, 0), (zm, other, 0), (zo, other, 0))
    from_above = ((zp, y2, 1), (zp, y2, 0), (zo, y2, 1), (zp, other, 1), (zo, other, 1))
    from_across = (
        (z, other, 0),
        (z, other, 1),
        (zm, other, 1),
        (zp, other, 0),
        (zm, other, 0),
        (zp, other, 1),
    )

    def share(n, src, zz, row, half):
        return pltpu.make_async_remote_copy(
            src_ref=src,
            dst_ref=piece(n, zz, row, half),
            send_sem=d2d_s.at[n],
            recv_sem=d2d_r.at[2 * n + (1 if zz is zo else 0)],
            device_id=(z, y, x, sib),
            device_id_type=MESH,
        )

    def arrive(n, sem, where, device):
        spot = piece(n, *where)
        cal_copy(n, spot, spot, sem, device).wait_recv()
        share(n, spot, *where).start()

    def below(n, k):
        arrive(n, k, from_below[k], down)

    def above(n, k):
        arrive(n, 5 + k, from_above[k], up)

    def beside(n, k):
        arrive(n, 10 + k, from_across[k], across)

    def own_copy(n):
        at = pl.ds((z * 2 + y2) * CAL_ROWS, CAL_ROWS)
        return pltpu.make_async_copy(
            cal_ref.at[:, pl.ds(STARTS[n], WIDTHS[n])],
            calbuf.at[at, lanes(n, c)],
            own_sem.at[n],
        )

    barrier = pltpu.get_barrier_semaphore()

    def greet(device):
        pl.semaphore_signal(barrier, inc=1, device_id=device, device_id_type=MESH)

    home = y // 2
    for device in (up, down, across, (z, y, x, sib), (z, 3 - y, x, 1)):
        greet(device)
    for device in ((z, y, xp, c), (z, y, xm, c)):
        greet(device)

    @pl.loop(0, OWNERS)
    def _(t):
        zs, ys = t // 4, t % 4

        @pl.when(jnp.logical_not((zs == z) & (ys == y) & (home == c)))
        def _():
            greet((zs, ys, x, home))


    def first(n):
        send_up(n, 0).start()
        send_down(n, 0).start()
        send_across(n, 0).start()

    def second(n):
        send_up(n, 1).start()
        send_down(n, 1).start()
        send_across(n, 1).start()

    def share_own(n):
        own_copy(n).start()
        for half in range(2):
            share(n, own_piece(n, half), z, y2, half).start()

    live = lax.broadcasted_iota(jnp.int32, (1, BLOCKS), 1) < count_ref[...]
    owner_row = jnp.where(live, owner_ref[...], -1)
    mask = owner_row == lax.broadcasted_iota(jnp.int32, (OWNERS, BLOCKS), 0)
    maskf = mask.astype(F32)
    steps = BLOCKS // 128
    stack = jnp.concatenate(
        [maskf[:, j * 128 : (j + 1) * 128] for j in range(steps)], axis=0
    ).astype(BF16)
    row_id = lax.broadcasted_iota(jnp.int32, (128, 128), 0)
    col_id = lax.broadcasted_iota(jnp.int32, (128, 128), 1)
    strict = (row_id < col_id).astype(F32).astype(BF16)
    before = jnp.dot(stack, strict, preferred_element_type=F32)
    total = jnp.dot(stack, jnp.ones((128, 128), BF16), preferred_element_type=F32)
    offset = jnp.zeros((OWNERS, 128), F32)
    for j in range(steps):
        rank = before[j * OWNERS : (j + 1) * OWNERS] + offset
        ranks[:, j * 128 : (j + 1) * 128] = jnp.where(
            mask[:, j * 128 : (j + 1) * 128], rank.astype(jnp.int32), -1
        )
        offset = offset + total[j * OWNERS : (j + 1) * OWNERS]

    sensor = sensor_ref[...]
    kid = lax.broadcasted_iota(jnp.int32, (16, BLOCKS), 0)
    key_rows = jnp.where(
        kid == 0,
        sensor // 128,
        jnp.where(kid == 1, sensor % 128, jnp.where(kid == 2, window_ref[...], 0)),
    )
    payload[LENGTH:PAYLOAD, :] = key_rows.astype(F32).astype(BF16)

    lane = lax.broadcasted_iota(jnp.int32, (CHUNK, LENGTH), 1)

    @pl.loop(0, BLOCKS // CHUNK)
    def _(i):
        at = pl.ds(pl.multiple_of(i * CHUNK, CHUNK), CHUNK)
        samples = values_ref[at, :].astype(F32)
        offsets = shifts_ref[at, :].astype(F32)

        def product(k):
            weight = jnp.maximum(0.0, 1.0 - jnp.abs(offsets - k)).astype(BF16)
            return weight.astype(F32) * samples

        result = product(0.0)
        result = result + jnp.where(lane >= 1, pltpu.roll(product(1.0), 1, 1), 0.0)
        result = result + jnp.where(
            lane < LENGTH - 1, pltpu.roll(product(-1.0), LENGTH - 1, 1), 0.0
        )
        payload[0:LENGTH, at] = result.T.astype(BF16)

    def destination(k):
        zd = (z + k // 4) % 4
        cd = k % 2
        yd = 2 * c + (k // 2) % 2
        yo = yd + cd * (3 - 2 * yd)
        return zd, yd, cd, zd * 4 + yo

    def message_copy(k, zd, yd, cd):
        return pltpu.make_async_remote_copy(
            src_ref=outbuf.at[k],
            dst_ref=rx.at[x, me_t],
            send_sem=a2a_s,
            recv_sem=a2a_r.at[k // 4],
            device_id=(zd, yd, x, cd),
            device_id_type=MESH,
        )

    low_lanes = lax.broadcasted_iota(jnp.int32, (1, 128), 1) < 64
    even = jnp.broadcast_to(y2, (1, 128)) == 0
    lead_slot = lax.broadcasted_iota(jnp.int16, (128, BLOCKS), 0)
    tail_slot = lax.broadcasted_iota(jnp.int16, (64, BLOCKS), 0) + 128
    fold = PAYLOAD // 2

    def hit(owner, slot):
        rank = ranks[pl.ds(owner, 1), :].astype(jnp.int16)
        return jnp.where(rank == slot, jnp.ones((), BF16), jnp.zeros((), BF16))

    def send_message(k):
        zd, yd, cd, _owner = destination(k)
        is_self = (zd == z) & (yd == y) & (cd == c)

        @pl.when(jnp.logical_not(is_self))
        def _():
            message_copy(k, zd, yd, cd).start()

        @pl.when(is_self)
        def _():
            pltpu.make_async_copy(
                outbuf.at[k], rx.at[x, me_t], a2a_r.at[k // 4]
            ).start()

    def messages(start, stop):
        @pl.loop(start, stop)
        def _(pair):
            k0, k1 = 2 * pair, 2 * pair + 1
            owner0, owner1 = destination(k0)[3], destination(k1)[3]
            pick = jnp.concatenate(
                [
                    hit(owner0, lead_slot),
                    hit(owner1, lead_slot),
                    hit(owner0, tail_slot),
                    hit(owner1, tail_slot),
                ],
                axis=0,
            )
            rows = lax.dot_general(payload[...], pick, NT, preferred_element_type=F32)
            outbuf[k0, 0:PAYLOAD, :] = rows[:, 0:128].astype(BF16)
            outbuf[k1, 0:PAYLOAD, :] = rows[:, 128:256].astype(BF16)
            tail = rows[:, 256:384]
            swapped = pltpu.roll(tail, 64, 1)
            near0 = jnp.where(even, tail[:fold], tail[fold:])
            far0 = jnp.where(even, swapped[fold:], swapped[:fold])
            near1 = jnp.where(even, swapped[:fold], swapped[fold:])
            far1 = jnp.where(even, tail[fold:], tail[:fold])
            outbuf[k0, PAYLOAD:MSG_ROWS, :] = jnp.where(low_lanes, near0, far0).astype(BF16)
            outbuf[k1, PAYLOAD:MSG_ROWS, :] = jnp.where(low_lanes, near1, far1).astype(BF16)
            send_message(k0)
            send_message(k1)

    def x_copy(src_x, group, sem, device):
        span = rx.at[src_x, pl.ds((z + 4 - group) % 4 * 4, 4)]
        return pltpu.make_async_remote_copy(
            src_ref=span,
            dst_ref=span,
            send_sem=x_s,
            recv_sem=x_r.at[sem],
            device_id=device,
            device_id_type=MESH,
        )

    right, left = (z, y, xp, c), (z, y, xm, c)

    def spread(group):
        span = rx.at[x, pl.ds((z + 4 - group) % 4 * 4, 4)]
        pltpu.make_async_copy(span, span, a2a_r.at[group]).wait()

        x_copy(x, group, group, right).start()
        x_copy(x, group, 4 + group, left).start()

    homed = home * c + (1 - home) * (1 - c)
    pl.semaphore_wait(barrier, OWNERS + 6 + 2 * c - homed)
    acc[...] = jnp.zeros_like(acc)

    def prepare(q):
        @pl.loop(0, OWNERS // 2)
        def _(p):
            m0 = rx.at[q, 2 * p]
            m1 = rx.at[q, 2 * p + 1]
            r0 = m0[PAYLOAD:MSG_ROWS, :].astype(F32)
            r1 = m1[PAYLOAD:MSG_ROWS, :].astype(F32)
            upper = jnp.where(low_lanes, r0, r1)
            lower = pltpu.roll(jnp.where(low_lanes, r1, r0), 64, 1)
            joint = jnp.concatenate([upper, lower], axis=0)
            tiles = (
                m0[0:PAYLOAD, :].astype(F32),
                m1[0:PAYLOAD, :].astype(F32),
                joint,
            )
            for n, tile in enumerate(tiles):
                at = pl.ds(pl.multiple_of(p * 384 + n * 128, 128), 128)
                slot_sensor[0:1, at] = (
                    tile[LENGTH : LENGTH + 1] * 128.0 + tile[LENGTH + 1 : LENGTH + 2]
                ).astype(jnp.int32)
                window = tile[LENGTH + 2 : LENGTH + 3]
                for w in range(WINDOWS):
                    placed[w * 128 : (w + 1) * 128, at] = jnp.where(
                        window == float(w), tile[0:LENGTH], 0.0
                    ).astype(BF16)

    def place(q, j):
        near = (slot_sensor[0:1, :] - j * WIDE).astype(jnp.int16)
        ids = lax.broadcasted_iota(jnp.int16, (WIDE, SLOTS), 0)
        hot[...] = jnp.where(ids == near, jnp.ones((), BF16), jnp.zeros((), BF16))
        block = lax.dot_general(placed[...], hot[...], NT, preferred_element_type=F32)
        at = pl.ds(pl.multiple_of(q * GROUP + j * WIDE, WIDE), WIDE)
        aligned[:, at] = block.astype(BF16)

    def shared(n, final):
        rows = 4 if final else 12
        spot = calbuf.at[pl.ds(0, rows * HALF), lanes(n, sib)]
        pltpu.make_async_copy(spot, spot, d2d_r.at[2 * n + final]).wait()

    def multiply(n, zz):
        depth = pl.ds(pl.multiple_of(zz * GROUP, GROUP), GROUP)
        return jnp.dot(
            aligned[:, depth], calbuf[depth, both(n)], preferred_element_type=F32
        )

    def early(n):
        own_copy(n).wait()
        shared(n, 0)

        @pl.loop(0, 3)
        def _(i):
            acc[:, both(n)] += multiply(n, (z + 3 * i - i // 2) % 4)

    def exchange(n, panel, sem_s, sem_r, device):
        at = pl.ds(STARTS[n], WIDTHS[n])
        return pltpu.make_async_remote_copy(
            src_ref=give.at[panel, :, at],
            dst_ref=take.at[sem_r, :, at],
            send_sem=ex_s.at[n * 2 + sem_s],
            recv_sem=ex_r.at[n * 2 + sem_r],
            device_id=device,
            device_id_type=MESH,
        )

    def late(n):
        shared(n, 1)
        total = acc[:, both(n)] + multiply(n, zo)
        width = WIDTHS[n]
        at = slice(STARTS[n], STARTS[n] + width)
        for panel in range(2):
            give[panel, :, at] = total[:, panel * width : (panel + 1) * width].astype(BF16)
        mine[:, at] = total[:, :width]

        @pl.when(c == 0)
        def _():
            exchange(n, 1, 0, 0, (z, y, x, 1)).start()

        @pl.when(c == 1)
        def _():
            exchange(n, 0, 0, 0, (z, 3 - y, x, 0)).start()
            exchange(n, 1, 1, 1, (z, 3 - y, x, 1)).start()

    def out_copy(n):
        return pltpu.make_async_copy(
            done.at[:, pl.ds(STARTS[n], WIDTHS[n])],
            out_ref.at[:, pl.ds(STARTS[n], WIDTHS[n])],
            out_sem.at[n],
        )

    def finish(n):
        at = slice(STARTS[n], STARTS[n] + WIDTHS[n])

        @pl.when(c == 0)
        def _():
            exchange(n, 0, 0, 0, (z, 3 - y, x, 1)).wait_recv()
            done[:, at] = (mine[:, at] + take[0, :, at].astype(F32)).astype(BF16)
            out_copy(n).start()
            exchange(n, 1, 0, 0, (z, y, x, 1)).wait_send()

        @pl.when(c == 1)
        def _():
            exchange(n, 0, 0, 0, (z, y, x, 0)).wait_recv()
            exchange(n, 1, 1, 1, (z, 3 - y, x, 1)).wait_recv()
            done[:, at] = (take[0, :, at].astype(F32) + take[1, :, at].astype(F32)).astype(BF16)
            out_copy(n).start()
            exchange(n, 0, 0, 0, (z, 3 - y, x, 0)).wait_send()
            exchange(n, 1, 1, 1, (z, 3 - y, x, 1)).wait_send()

    messages(0, 8)
    send_up(0, 0).start()
    send_down(0, 0).start()
    send_across(0, 0).start()
    share_own(0)
    spread(0)
    spread(1)
    send_up(0, 1).start()
    send_up(1, 0).start()
    share_own(1)
    send_down(0, 1).start()
    send_down(1, 0).start()
    send_across(0, 1).start()
    send_across(1, 0).start()
    spread(2)
    spread(3)
    prepare(x)
    send_up(1, 1).start()
    send_down(1, 1).start()
    send_across(1, 1).start()
    place(x, 0)
    above(0, 0)
    send_down(0, 2).start()
    below(0, 0)
    send_up(0, 2).start()
    beside(0, 0)
    send_up(0, 3).start()
    send_down(2, 0).start()
    share_own(2)
    send_across(2, 0).start()
    send_across(2, 1).start()
    place(x, 1)
    beside(0, 1)
    send_down(0, 3).start()
    above(0, 1)
    send_across(0, 3).start()
    below(0, 1)
    send_across(0, 2).start()
    above(1, 0)
    send_down(1, 2).start()
    beside(1, 0)
    send_up(1, 3).start()
    below(1, 0)
    send_up(1, 2).start()
    x_copy(xm, 0, 0, left).wait_recv()
    x_copy(xm, 0, 8, right).start()
    x_copy(xm, 1, 1, left).wait_recv()
    x_copy(xm, 1, 9, right).start()
    x_copy(xp, 2, 6, right).wait_recv()
    x_copy(xp, 2, 10, left).start()
    x_copy(xp, 3, 7, right).wait_recv()
    x_copy(xp, 3, 11, left).start()
    below(1, 1)
    send_across(1, 2).start()
    above(1, 1)
    send_across(1, 3).start()
    beside(1, 1)
    send_down(1, 3).start()
    send_up(2, 0).start()
    x_copy(xm, 2, 2, left).wait_recv()
    x_copy(xm, 3, 3, left).wait_recv()
    prepare(xm)
    place(xm, 0)
    below(0, 3)
    send_up(0, 4).start()
    below(0, 2)
    above(0, 2)
    above(2, 0)
    send_down(2, 2).start()
    send_across(2, 5).start()
    beside(2, 0)
    beside(2, 1)
    send_up(2, 1).start()
    send_up(3, 0).start()
    share_own(3)
    send_down(2, 1).start()
    send_down(3, 0).start()
    place(xm, 1)
    below(1, 3)
    send_up(1, 4).start()
    below(1, 2)
    above(0, 3)
    send_down(0, 4).start()
    above(1, 2)
    above(1, 3)
    send_down(1, 4).start()
    below(2, 0)
    send_up(2, 2).start()
    send_across(2, 4).start()
    beside(0, 3)
    beside(0, 2)
    x_copy(xp, 0, 4, right).wait_recv()
    x_copy(xp, 1, 5, right).wait_recv()
    prepare(xp)
    send_across(3, 0).start()
    place(xp, 0)
    beside(1, 2)
    beside(1, 3)
    place(xp, 1)
    beside(2, 5)
    send_down(2, 4).start()
    send_across(3, 1).start()
    x_copy(xo, 0, 8, left).wait_recv()
    x_copy(xo, 1, 9, left).wait_recv()
    x_copy(xo, 2, 10, right).wait_recv()
    x_copy(xo, 3, 11, right).wait_recv()
    prepare(xo)
    send_up(3, 1).start()
    place(xo, 0)
    beside(2, 4)
    send_up(2, 4).start()
    beside(3, 0)
    send_up(3, 3).start()
    below(2, 1)
    send_across(2, 2).start()
    below(3, 0)
    send_up(3, 2).start()
    below(0, 4)
    above(3, 0)
    send_down(3, 2).start()
    above(2, 1)
    send_across(2, 3).start()
    above(2, 2)
    send_down(3, 1).start()
    place(xo, 1)
    beside(3, 1)
    send_down(3, 3).start()
    below(1, 4)
    below(2, 2)
    above(0, 4)
    above(1, 4)
    early(0)
    late(0)
    above(2, 4)
    early(1)
    below(3, 1)
    send_across(3, 2).start()
    late(1)
    beside(2, 3)
    beside(2, 2)
    early(2)
    above(3, 1)
    send_across(3, 3).start()
    above(3, 2)
    above(3, 3)
    send_down(3, 4).start()
    below(3, 2)
    below(3, 3)
    send_up(3, 4).start()
    below(2, 4)
    late(2)
    beside(3, 2)
    beside(3, 3)
    below(3, 4)
    above(3, 4)
    early(3)
    late(3)
    def sent(ref, sem):
        pltpu.make_async_copy(ref, ref, sem).wait()

    for n in range(PARTS):
        sent(calbuf.at[pl.ds(0, 14 * HALF), lanes(n, c)], cal_s.at[n])
        sent(calbuf.at[:, lanes(n, c)], d2d_s.at[n])
    sent(rx.at[pl.ds(0, 3)], x_s)

    @pl.when(home == c)
    def _():
        sent(outbuf.at[pl.ds(0, OWNERS - 1)], a2a_s)

    @pl.when(home != c)
    def _():
        sent(outbuf, a2a_s)

    finish(0)
    finish(1)
    finish(2)
    finish(3)
    for n in range(PARTS):
        out_copy(n).wait()


def per_device(
    block_values, block_shifts, block_sensor, block_window, block_owner, block_counts, calibration
):
    vmem = pl.BlockSpec(memory_space=pltpu.VMEM)
    return pl.pallas_call(
        kernel,
        out_shape=jax.ShapeDtypeStruct((ROWS, COLS), BF16),
        in_specs=[vmem] * 6 + [pl.BlockSpec(memory_space=pl.ANY)],
        out_specs=pl.BlockSpec(memory_space=pl.ANY),
        scratch_shapes=[
            pltpu.VMEM((OWNERS, BLOCKS), jnp.int32),
            pltpu.VMEM((PAYLOAD, BLOCKS), BF16),
            pltpu.VMEM((OWNERS, MSG_ROWS, LENGTH), BF16),
            pltpu.VMEM((4, OWNERS, MSG_ROWS, LENGTH), BF16),
            pltpu.VMEM((ROWS, SLOTS), BF16),
            pltpu.VMEM((8, SLOTS), jnp.int32),
            pltpu.VMEM((WIDE, SLOTS), BF16),
            pltpu.VMEM((ROWS, DEPTH), BF16),
            pltpu.VMEM((DEPTH, 2 * COLS), BF16),
            pltpu.VMEM((ROWS, 2 * COLS), F32),
            pltpu.VMEM((ROWS, COLS), F32),
            pltpu.VMEM((2, ROWS, COLS), BF16),
            pltpu.VMEM((2, ROWS, COLS), BF16),
            pltpu.VMEM((ROWS, COLS), BF16),
            pltpu.SemaphoreType.DMA,
            pltpu.SemaphoreType.DMA((4,)),
            pltpu.SemaphoreType.DMA,
            pltpu.SemaphoreType.DMA((12,)),
            pltpu.SemaphoreType.DMA((PARTS,)),
            pltpu.SemaphoreType.DMA((PARTS * MOVES,)),
            pltpu.SemaphoreType.DMA((PARTS,)),
            pltpu.SemaphoreType.DMA((PARTS * 2,)),
            pltpu.SemaphoreType.DMA((PARTS * 2,)),
            pltpu.SemaphoreType.DMA((PARTS * 2,)),
            pltpu.SemaphoreType.DMA((PARTS,)),
            pltpu.SemaphoreType.DMA((PARTS,)),
        ],
        compiler_params=pltpu.CompilerParams(
            collective_id=0, has_side_effects=True, vmem_limit_bytes=60 * 1024 * 1024
        ),
    )(
        block_values[0],
        block_shifts[0],
        block_sensor,
        block_window,
        block_owner.reshape(1, BLOCKS),
        block_counts,
        calibration,
    )


def solution(mesh):
    torus = Mesh(mesh.devices.reshape(4, 4, 4, 2), ("z", "y", "x", "c"))
    tm, col = ("z", "y"), ("x", "c")
    in_specs = (
        P(col, tm, None),
        P(col, tm, None),
        P(col, tm),
        P(col, tm),
        P(col, tm, None),
        P(col, tm),
        P(tm, col),
    )
    return jax.shard_map(
        per_device, mesh=torus, in_specs=in_specs, out_specs=P(tm, col), check_vma=False
    )
```

```python
import jax
import jax.numpy as jnp
from jax import lax
from jax.experimental import pallas as pl
from jax.experimental.pallas import tpu as pltpu
from jax.sharding import Mesh
from jax.sharding import PartitionSpec as P

MESH = pl.DeviceIdType.MESH
F32 = jnp.float32
BF16 = jnp.bfloat16

LENGTH = 128
BLOCKS = 2048
OWNERS = 16
CAPACITY = 192
WINDOWS = 4
GROUP = 2048
ROWS = 512
COLS = 512
CAL_ROWS = 1024
HALF = CAL_ROWS // 2
WIDTHS = (128, 128, 128, 128)
PARTS = len(WIDTHS)
STARTS = tuple(sum(WIDTHS[:n]) for n in range(PARTS))
MOVES = 16
EASED = (2,)
DEPTH = 4 * GROUP
PAYLOAD = LENGTH + 16
MSG_ROWS = PAYLOAD + PAYLOAD // 2
SLOTS = OWNERS * CAPACITY
CHUNK = 256
WIDE = 1024
NT = (((1,), (1,)), ((), ()))


def kernel(
    values_ref,
    shifts_ref,
    sensor_ref,
    window_ref,
    owner_ref,
    count_ref,
    cal_ref,
    out_ref,
    ranks,
    payload,
    outbuf,
    rx,
    placed,
    slot_sensor,
    hot,
    aligned,
    calbuf,
    acc,
    mine,
    give,
    take,
    done,
    a2a_s,
    a2a_r,
    x_s,
    x_r,
    cal_s,
    cal_r,
    d2d_s,
    d2d_r,
    ex_s,
    ex_r,
    own_sem,
    out_sem,
):
    z, y, x, c = (lax.axis_index(name) for name in ("z", "y", "x", "c"))
    zp, zm, zo = (z + 1) % 4, (z + 3) % 4, (z + 2) % 4
    xp, xm, xo = (x + 1) % 4, (x + 3) % 4, (x + 2) % 4
    y2 = y % 2
    yq = y + 1 - 2 * y2
    sib = 1 - c
    me_t = z * 4 + y

    def lanes(n, core):
        at = 2 * STARTS[n] + core * WIDTHS[n]
        return pl.ds(pl.multiple_of(at, 128), WIDTHS[n])

    def both(n):
        return slice(2 * STARTS[n], 2 * STARTS[n] + 2 * WIDTHS[n])

    def piece(n, zz, row, half):
        at = pl.ds((zz * 2 + row) * CAL_ROWS + half * HALF, HALF)
        return calbuf.at[at, lanes(n, c)]

    def own_piece(n, half):
        return cal_ref.at[pl.ds(half * HALF, HALF), pl.ds(STARTS[n], WIDTHS[n])]

    def cal_copy(n, src, dst, sem, device):
        return pltpu.make_async_remote_copy(
            src_ref=src,
            dst_ref=dst,
            send_sem=cal_s.at[n],
            recv_sem=cal_r.at[n * MOVES + sem],
            device_id=device,
            device_id_type=MESH,
        )

    up, down, across = (zp, y, x, c), (zm, y, x, c), (z, yq, x, c)

    def relay(n, sem, spot, device):
        own = spot[0] is z and spot[1] is y2
        src = own_piece(n, spot[2]) if own else piece(n, *spot)
        return cal_copy(n, src, piece(n, *spot), sem, device)

    other = 1 - y2
    go_up = ((z, y2, 0), (z, y2, 1), (zm, y2, 0), (z, other, 0), (zm, other, 0))
    go_down = ((z, y2, 1), (z, y2, 0), (zp, y2, 1), (z, other, 1), (zp, other, 1))
    go_across = (
        (z, y2, 0),
        (z, y2, 1),
        (zm, y2, 1),
        (zp, y2, 0),
        (zm, y2, 0),
        (zp, y2, 1),
    )

    def send_up(n, k):
        return relay(n, k, go_up[k], up)

    def send_down(n, k):
        return relay(n, 5 + k, go_down[k], down)

    def send_across(n, k):
        return relay(n, 10 + k, go_across[k], across)

    from_below = ((zm, y2, 0), (zm, y2, 1), (zo, y2, 0), (zm, other, 0), (zo, other, 0))
    from_above = ((zp, y2, 1), (zp, y2, 0), (zo, y2, 1), (zp, other, 1), (zo, other, 1))
    from_across = (
        (z, other, 0),
        (z, other, 1),
        (zm, other, 1),
        (zp, other, 0),
        (zm, other, 0),
        (zp, other, 1),
    )

    def share(n, src, zz, row, half):
        return pltpu.make_async_remote_copy(
            src_ref=src,
            dst_ref=piece(n, zz, row, half),
            send_sem=d2d_s.at[n],
            recv_sem=d2d_r.at[2 * n + (1 if zz is zo else 0)],
            device_id=(z, y, x, sib),
            device_id_type=MESH,
        )

    def arrive(n, sem, where, device):
        spot = piece(n, *where)
        cal_copy(n, spot, spot, sem, device).wait_recv()
        share(n, spot, *where).start()

    def below(n, k):
        arrive(n, k, from_below[k], down)

    def above(n, k):
        arrive(n, 5 + k, from_above[k], up)

    def beside(n, k):
        arrive(n, 10 + k, from_across[k], across)

    def own_copy(n):
        at = pl.ds((z * 2 + y2) * CAL_ROWS, CAL_ROWS)
        return pltpu.make_async_copy(
            cal_ref.at[:, pl.ds(STARTS[n], WIDTHS[n])],
            calbuf.at[at, lanes(n, c)],
            own_sem.at[n],
        )

    barrier = pltpu.get_barrier_semaphore()

    def greet(device):
        pl.semaphore_signal(barrier, inc=1, device_id=device, device_id_type=MESH)

    home = y // 2
    for device in (up, down, across, (z, y, x, sib), (z, 3 - y, x, 1)):
        greet(device)
    for device in ((z, y, xp, c), (z, y, xm, c)):
        greet(device)

    @pl.loop(0, OWNERS)
    def _(t):
        zs, ys = t // 4, t % 4

        @pl.when(jnp.logical_not((zs == z) & (ys == y) & (home == c)))
        def _():
            greet((zs, ys, x, home))


    def first(n):
        send_up(n, 0).start()
        send_down(n, 0).start()
        send_across(n, 0).start()

    def second(n):
        send_up(n, 1).start()
        send_down(n, 1).start()
        send_across(n, 1).start()

    def share_own(n):
        own_copy(n).start()
        for half in range(2):
            share(n, own_piece(n, half), z, y2, half).start()

    live = lax.broadcasted_iota(jnp.int32, (1, BLOCKS), 1) < count_ref[...]
    owner_row = jnp.where(live, owner_ref[...], -1)
    mask = owner_row == lax.broadcasted_iota(jnp.int32, (OWNERS, BLOCKS), 0)
    maskf = mask.astype(F32)
    steps = BLOCKS // 128
    stack = jnp.concatenate(
        [maskf[:, j * 128 : (j + 1) * 128] for j in range(steps)], axis=0
    ).astype(BF16)
    row_id = lax.broadcasted_iota(jnp.int32, (128, 128), 0)
    col_id = lax.broadcasted_iota(jnp.int32, (128, 128), 1)
    strict = (row_id < col_id).astype(F32).astype(BF16)
    before = jnp.dot(stack, strict, preferred_element_type=F32)
    total = jnp.dot(stack, jnp.ones((128, 128), BF16), preferred_element_type=F32)
    offset = jnp.zeros((OWNERS, 128), F32)
    for j in range(steps):
        rank = before[j * OWNERS : (j + 1) * OWNERS] + offset
        ranks[:, j * 128 : (j + 1) * 128] = jnp.where(
            mask[:, j * 128 : (j + 1) * 128], rank.astype(jnp.int32), -1
        )
        offset = offset + total[j * OWNERS : (j + 1) * OWNERS]

    sensor = sensor_ref[...]
    kid = lax.broadcasted_iota(jnp.int32, (16, BLOCKS), 0)
    key_rows = jnp.where(
        kid == 0,
        sensor // 128,
        jnp.where(kid == 1, sensor % 128, jnp.where(kid == 2, window_ref[...], 0)),
    )
    payload[LENGTH:PAYLOAD, :] = key_rows.astype(F32).astype(BF16)

    lane = lax.broadcasted_iota(jnp.int32, (CHUNK, LENGTH), 1)

    @pl.loop(0, BLOCKS // CHUNK)
    def _(i):
        at = pl.ds(pl.multiple_of(i * CHUNK, CHUNK), CHUNK)
        samples = values_ref[at, :].astype(F32)
        offsets = shifts_ref[at, :].astype(F32)

        def product(k):
            weight = jnp.maximum(0.0, 1.0 - jnp.abs(offsets - k)).astype(BF16)
            return weight.astype(F32) * samples

        result = product(0.0)
        result = result + jnp.where(lane >= 1, pltpu.roll(product(1.0), 1, 1), 0.0)
        result = result + jnp.where(
            lane < LENGTH - 1, pltpu.roll(product(-1.0), LENGTH - 1, 1), 0.0
        )
        payload[0:LENGTH, at] = result.T.astype(BF16)

    def destination(k):
        zd = (z + k // 4) % 4
        cd = k % 2
        yd = 2 * c + (k // 2) % 2
        yo = yd + cd * (3 - 2 * yd)
        return zd, yd, cd, zd * 4 + yo

    def message_copy(k, zd, yd, cd):
        return pltpu.make_async_remote_copy(
            src_ref=outbuf.at[k],
            dst_ref=rx.at[x, me_t],
            send_sem=a2a_s,
            recv_sem=a2a_r.at[k // 4],
            device_id=(zd, yd, x, cd),
            device_id_type=MESH,
        )

    low_lanes = lax.broadcasted_iota(jnp.int32, (1, 128), 1) < 64
    even = jnp.broadcast_to(y2, (1, 128)) == 0
    lead_slot = lax.broadcasted_iota(jnp.int16, (128, BLOCKS), 0)
    tail_slot = lax.broadcasted_iota(jnp.int16, (64, BLOCKS), 0) + 128
    fold = PAYLOAD // 2

    def hit(owner, slot):
        rank = ranks[pl.ds(owner, 1), :].astype(jnp.int16)
        return jnp.where(rank == slot, jnp.ones((), BF16), jnp.zeros((), BF16))

    def send_message(k):
        zd, yd, cd, _owner = destination(k)
        is_self = (zd == z) & (yd == y) & (cd == c)

        @pl.when(jnp.logical_not(is_self))
        def _():
            message_copy(k, zd, yd, cd).start()

        @pl.when(is_self)
        def _():
            pltpu.make_async_copy(
                outbuf.at[k], rx.at[x, me_t], a2a_r.at[k // 4]
            ).start()

    def messages(start, stop):
        @pl.loop(start, stop)
        def _(pair):
            k0, k1 = 2 * pair, 2 * pair + 1
            owner0, owner1 = destination(k0)[3], destination(k1)[3]
            pick = jnp.concatenate(
                [
                    hit(owner0, lead_slot),
                    hit(owner1, lead_slot),
                    hit(owner0, tail_slot),
                    hit(owner1, tail_slot),
                ],
                axis=0,
            )
            rows = lax.dot_general(payload[...], pick, NT, preferred_element_type=F32)
            outbuf[k0, 0:PAYLOAD, :] = rows[:, 0:128].astype(BF16)
            outbuf[k1, 0:PAYLOAD, :] = rows[:, 128:256].astype(BF16)
            tail = rows[:, 256:384]
            swapped = pltpu.roll(tail, 64, 1)
            near0 = jnp.where(even, tail[:fold], tail[fold:])
            far0 = jnp.where(even, swapped[fold:], swapped[:fold])
            near1 = jnp.where(even, swapped[:fold], swapped[fold:])
            far1 = jnp.where(even, tail[fold:], tail[:fold])
            outbuf[k0, PAYLOAD:MSG_ROWS, :] = jnp.where(low_lanes, near0, far0).astype(BF16)
            outbuf[k1, PAYLOAD:MSG_ROWS, :] = jnp.where(low_lanes, near1, far1).astype(BF16)
            send_message(k0)
            send_message(k1)

    def x_copy(src_x, group, sem, device):
        span = rx.at[src_x, pl.ds((z + 4 - group) % 4 * 4, 4)]
        return pltpu.make_async_remote_copy(
            src_ref=span,
            dst_ref=span,
            send_sem=x_s,
            recv_sem=x_r.at[sem],
            device_id=device,
            device_id_type=MESH,
        )

    right, left = (z, y, xp, c), (z, y, xm, c)

    def spread(group):
        span = rx.at[x, pl.ds((z + 4 - group) % 4 * 4, 4)]
        pltpu.make_async_copy(span, span, a2a_r.at[group]).wait()

        x_copy(x, group, group, right).start()
        x_copy(x, group, 4 + group, left).start()

    homed = home * c + (1 - home) * (1 - c)
    pl.semaphore_wait(barrier, OWNERS + 6 + 2 * c - homed)
    acc[...] = jnp.zeros_like(acc)

    def prepare(q):
        @pl.loop(0, OWNERS // 2)
        def _(p):
            m0 = rx.at[q, 2 * p]
            m1 = rx.at[q, 2 * p + 1]
            r0 = m0[PAYLOAD:MSG_ROWS, :].astype(F32)
            r1 = m1[PAYLOAD:MSG_ROWS, :].astype(F32)
            upper = jnp.where(low_lanes, r0, r1)
            lower = pltpu.roll(jnp.where(low_lanes, r1, r0), 64, 1)
            joint = jnp.concatenate([upper, lower], axis=0)
            tiles = (
                m0[0:PAYLOAD, :].astype(F32),
                m1[0:PAYLOAD, :].astype(F32),
                joint,
            )
            for n, tile in enumerate(tiles):
                at = pl.ds(pl.multiple_of(p * 384 + n * 128, 128), 128)
                slot_sensor[0:1, at] = (
                    tile[LENGTH : LENGTH + 1] * 128.0 + tile[LENGTH + 1 : LENGTH + 2]
                ).astype(jnp.int32)
                window = tile[LENGTH + 2 : LENGTH + 3]
                for w in range(WINDOWS):
                    placed[w * 128 : (w + 1) * 128, at] = jnp.where(
                        window == float(w), tile[0:LENGTH], 0.0
                    ).astype(BF16)

    def place(q, j):
        near = (slot_sensor[0:1, :] - j * WIDE).astype(jnp.int16)
        ids = lax.broadcasted_iota(jnp.int16, (WIDE, SLOTS), 0)
        hot[...] = jnp.where(ids == near, jnp.ones((), BF16), jnp.zeros((), BF16))
        block = lax.dot_general(placed[...], hot[...], NT, preferred_element_type=F32)
        at = pl.ds(pl.multiple_of(q * GROUP + j * WIDE, WIDE), WIDE)
        aligned[:, at] = block.astype(BF16)

    def shared(n, final):
        rows = 4 if final else 12
        spot = calbuf.at[pl.ds(0, rows * HALF), lanes(n, sib)]
        pltpu.make_async_copy(spot, spot, d2d_r.at[2 * n + final]).wait()

    def multiply(n, zz):
        depth = pl.ds(pl.multiple_of(zz * GROUP, GROUP), GROUP)
        return jnp.dot(
            aligned[:, depth], calbuf[depth, both(n)], preferred_element_type=F32
        )

    def early(n):
        own_copy(n).wait()
        shared(n, 0)

        @pl.loop(0, 3)
        def _(i):
            acc[:, both(n)] += multiply(n, (z + 3 * i - i // 2) % 4)

    def exchange(n, panel, sem_s, sem_r, device):
        at = pl.ds(STARTS[n], WIDTHS[n])
        return pltpu.make_async_remote_copy(
            src_ref=give.at[panel, :, at],
            dst_ref=take.at[sem_r, :, at],
            send_sem=ex_s.at[n * 2 + sem_s],
            recv_sem=ex_r.at[n * 2 + sem_r],
            device_id=device,
            device_id_type=MESH,
        )

    def late(n):
        shared(n, 1)
        total = acc[:, both(n)] + multiply(n, zo)
        width = WIDTHS[n]
        at = slice(STARTS[n], STARTS[n] + width)
        for panel in range(2):
            give[panel, :, at] = total[:, panel * width : (panel + 1) * width].astype(BF16)
        mine[:, at] = total[:, :width]

        @pl.when(c == 0)
        def _():
            exchange(n, 1, 0, 0, (z, y, x, 1)).start()

        @pl.when(c == 1)
        def _():
            exchange(n, 0, 0, 0, (z, 3 - y, x, 0)).start()
            exchange(n, 1, 1, 1, (z, 3 - y, x, 1)).start()

    def out_copy(n):
        return pltpu.make_async_copy(
            done.at[:, pl.ds(STARTS[n], WIDTHS[n])],
            out_ref.at[:, pl.ds(STARTS[n], WIDTHS[n])],
            out_sem.at[n],
        )

    def finish(n):
        at = slice(STARTS[n], STARTS[n] + WIDTHS[n])

        @pl.when(c == 0)
        def _():
            exchange(n, 0, 0, 0, (z, 3 - y, x, 1)).wait_recv()
            done[:, at] = (mine[:, at] + take[0, :, at].astype(F32)).astype(BF16)
            out_copy(n).start()
            exchange(n, 1, 0, 0, (z, y, x, 1)).wait_send()

        @pl.when(c == 1)
        def _():
            exchange(n, 0, 0, 0, (z, y, x, 0)).wait_recv()
            exchange(n, 1, 1, 1, (z, 3 - y, x, 1)).wait_recv()
            done[:, at] = (take[0, :, at].astype(F32) + take[1, :, at].astype(F32)).astype(BF16)
            out_copy(n).start()
            exchange(n, 0, 0, 0, (z, 3 - y, x, 0)).wait_send()
            exchange(n, 1, 1, 1, (z, 3 - y, x, 1)).wait_send()

    messages(0, 8)
    send_up(0, 0).start()
    send_down(0, 0).start()
    send_across(0, 0).start()
    share_own(0)
    spread(0)
    spread(1)
    send_up(0, 1).start()
    send_up(1, 0).start()
    share_own(1)
    send_down(0, 1).start()
    send_down(1, 0).start()
    send_across(0, 1).start()
    send_across(1, 0).start()
    spread(2)
    spread(3)
    prepare(x)
    send_up(1, 1).start()
    send_down(1, 1).start()
    send_across(1, 1).start()
    place(x, 0)
    above(0, 0)
    send_down(0, 2).start()
    below(0, 0)
    send_up(0, 2).start()
    beside(0, 0)
    send_up(0, 3).start()
    send_down(2, 0).start()
    share_own(2)
    send_across(2, 0).start()
    send_across(2, 1).start()
    place(x, 1)
    beside(0, 1)
    send_down(0, 3).start()
    above(0, 1)
    send_across(0, 3).start()
    below(0, 1)
    send_across(0, 2).start()
    above(1, 0)
    send_down(1, 2).start()
    beside(1, 0)
    send_up(1, 3).start()
    below(1, 0)
    send_up(1, 2).start()
    x_copy(xm, 0, 0, left).wait_recv()
    x_copy(xm, 0, 8, right).start()
    x_copy(xm, 1, 1, left).wait_recv()
    x_copy(xm, 1, 9, right).start()
    x_copy(xp, 2, 6, right).wait_recv()
    x_copy(xp, 2, 10, left).start()
    x_copy(xp, 3, 7, right).wait_recv()
    x_copy(xp, 3, 11, left).start()
    below(1, 1)
    send_across(1, 2).start()
    above(1, 1)
    send_across(1, 3).start()
    beside(1, 1)
    send_down(1, 3).start()
    send_up(2, 0).start()
    x_copy(xm, 2, 2, left).wait_recv()
    x_copy(xm, 3, 3, left).wait_recv()
    prepare(xm)
    place(xm, 0)
    below(0, 3)
    send_up(0, 4).start()
    below(0, 2)
    above(0, 2)
    above(2, 0)
    send_down(2, 2).start()
    send_across(2, 5).start()
    beside(2, 0)
    beside(2, 1)
    send_up(2, 1).start()
    send_up(3, 0).start()
    share_own(3)
    send_down(2, 1).start()
    send_down(3, 0).start()
    place(xm, 1)
    below(1, 3)
    send_up(1, 4).start()
    above(0, 3)
    send_down(0, 4).start()
    x_copy(xp, 0, 4, right).wait_recv()
    x_copy(xp, 1, 5, right).wait_recv()
    prepare(xp)
    send_across(3, 0).start()
    place(xp, 0)
    above(1, 3)
    send_down(1, 4).start()
    below(2, 0)
    send_up(2, 2).start()
    send_across(2, 4).start()
    send_up(3, 1).start()
    send_down(3, 1).start()
    send_across(3, 1).start()
    below(1, 2)
    above(1, 2)
    beside(0, 3)
    beside(0, 2)
    beside(1, 2)
    beside(1, 3)
    place(xp, 1)
    beside(2, 5)
    send_down(2, 4).start()
    x_copy(xo, 0, 8, left).wait_recv()
    x_copy(xo, 1, 9, left).wait_recv()
    x_copy(xo, 2, 10, right).wait_recv()
    x_copy(xo, 3, 11, right).wait_recv()
    prepare(xo)
    place(xo, 0)
    beside(2, 4)
    send_up(2, 4).start()
    beside(3, 0)
    send_up(3, 3).start()
    below(2, 1)
    send_across(2, 2).start()
    below(3, 0)
    send_up(3, 2).start()
    below(0, 4)
    above(3, 0)
    send_down(3, 2).start()
    above(2, 1)
    send_across(2, 3).start()
    above(2, 2)
    place(xo, 1)
    beside(3, 1)
    send_down(3, 3).start()
    below(1, 4)
    below(2, 2)
    above(0, 4)
    early(0)
    below(3, 1)
    send_across(3, 2).start()
    above(3, 1)
    send_across(3, 3).start()
    above(1, 4)
    late(0)
    early(1)
    late(1)
    below(3, 3)
    send_up(3, 4).start()
    above(3, 3)
    send_down(3, 4).start()
    above(2, 4)
    beside(2, 3)
    beside(2, 2)
    below(2, 4)
    early(2)
    above(3, 2)
    below(3, 2)
    late(2)
    beside(3, 2)
    beside(3, 3)
    below(3, 4)
    above(3, 4)
    early(3)
    late(3)

    def sent(ref, sem):
        pltpu.make_async_copy(ref, ref, sem).wait()

    for n in range(PARTS):
        sent(calbuf.at[pl.ds(0, 14 * HALF), lanes(n, c)], cal_s.at[n])
        sent(calbuf.at[:, lanes(n, c)], d2d_s.at[n])
    sent(rx.at[pl.ds(0, 3)], x_s)

    @pl.when(home == c)
    def _():
        sent(outbuf.at[pl.ds(0, OWNERS - 1)], a2a_s)

    @pl.when(home != c)
    def _():
        sent(outbuf, a2a_s)

    finish(0)
    finish(1)
    finish(2)
    finish(3)
    for n in range(PARTS):
        out_copy(n).wait()


def per_device(
    block_values, block_shifts, block_sensor, block_window, block_owner, block_counts, calibration
):
    vmem = pl.BlockSpec(memory_space=pltpu.VMEM)
    return pl.pallas_call(
        kernel,
        out_shape=jax.ShapeDtypeStruct((ROWS, COLS), BF16),
        in_specs=[vmem] * 6 + [pl.BlockSpec(memory_space=pl.ANY)],
        out_specs=pl.BlockSpec(memory_space=pl.ANY),
        scratch_shapes=[
            pltpu.VMEM((OWNERS, BLOCKS), jnp.int32),
            pltpu.VMEM((PAYLOAD, BLOCKS), BF16),
            pltpu.VMEM((OWNERS, MSG_ROWS, LENGTH), BF16),
            pltpu.VMEM((4, OWNERS, MSG_ROWS, LENGTH), BF16),
            pltpu.VMEM((ROWS, SLOTS), BF16),
            pltpu.VMEM((8, SLOTS), jnp.int32),
            pltpu.VMEM((WIDE, SLOTS), BF16),
            pltpu.VMEM((ROWS, DEPTH), BF16),
            pltpu.VMEM((DEPTH, 2 * COLS), BF16),
            pltpu.VMEM((ROWS, 2 * COLS), F32),
            pltpu.VMEM((ROWS, COLS), F32),
            pltpu.VMEM((2, ROWS, COLS), BF16),
            pltpu.VMEM((2, ROWS, COLS), BF16),
            pltpu.VMEM((ROWS, COLS), BF16),
            pltpu.SemaphoreType.DMA,
            pltpu.SemaphoreType.DMA((4,)),
            pltpu.SemaphoreType.DMA,
            pltpu.SemaphoreType.DMA((12,)),
            pltpu.SemaphoreType.DMA((PARTS,)),
            pltpu.SemaphoreType.DMA((PARTS * MOVES,)),
            pltpu.SemaphoreType.DMA((PARTS,)),
            pltpu.SemaphoreType.DMA((PARTS * 2,)),
            pltpu.SemaphoreType.DMA((PARTS * 2,)),
            pltpu.SemaphoreType.DMA((PARTS * 2,)),
            pltpu.SemaphoreType.DMA((PARTS,)),
            pltpu.SemaphoreType.DMA((PARTS,)),
        ],
        compiler_params=pltpu.CompilerParams(
            collective_id=0, has_side_effects=True, vmem_limit_bytes=60 * 1024 * 1024
        ),
    )(
        block_values[0],
        block_shifts[0],
        block_sensor,
        block_window,
        block_owner.reshape(1, BLOCKS),
        block_counts,
        calibration,
    )


def solution(mesh):
    torus = Mesh(mesh.devices.reshape(4, 4, 4, 2), ("z", "y", "x", "c"))
    tm, col = ("z", "y"), ("x", "c")
    in_specs = (
        P(col, tm, None),
        P(col, tm, None),
        P(col, tm),
        P(col, tm),
        P(col, tm, None),
        P(col, tm),
        P(tm, col),
    )
    return jax.shard_map(
        per_device, mesh=torus, in_specs=in_specs, out_specs=P(tm, col), check_vma=False
    )
```
